32 devices in a mesh: col: 8 (over z, x), row: 4 (over y, core).
Axes of the slice: x: 2, y: 2, z: 4, core: 2. Of those that a mesh axis runs over, the one named last changes fastest.
Arguments:
- vorticity: float32 [2, 8, 1024, 2048], P(None, 'row', 'col'), may hold values from -0.0017578125 to 0.0017578125
- divergence: float32 [2, 8, 1024, 2048], P(None, 'row', 'col'), may hold values from -0.0017578125 to 0.0017578125
- trunc_cut: int32 [1024], P('col'), may hold values from -1 to 1023, as said below
- level_slot: int32 [8], replicated, may hold values from 0 to 7, each once
Outputs:
- u_wind: float32 [8, 2048, 2048], P(None, ('col', 'row'))
- v_wind: float32 [8, 2048, 2048], P(None, ('col', 'row'))
- u_slope: float32 [8, 2048, 2048], P(None, ('col', 'row'))
- v_slope: float32 [8, 2048, 2048], P(None, ('col', 'row'))
The draws below stay inside these ranges and needn't reach their ends.
Inputs may be any that keep to these rules, and one draw needn't show every extreme that they name: trunc_cut never rises with m, is 1023 at m = 0 and -1 (nothing kept) at the last m. level_slot is a permutation of the model levels.
All inputs are finite; a program needn't handle non-finite values.
Results may differ from the reference program's by a relative error of at most 0.0001.
Values sent between devices are 32-bit elements; how exact they have to be, the bound alone decides.
No kernel may reach another device: no remote copies, remote signals or barrier semaphores. Data moves between devices by JAX's collectives and lax.ppermute only.
A program may use at most 128 MiB of HBM per device.

```python
import math
import jax
import jax.numpy as jnp
from jax import lax

NX = 2048
NY = 2048
MX = 1024
LEVELS = 8


def draw_trunc_cut(key, part):
    first_key = jax.random.fold_in(key, 11)
    second_key = jax.random.fold_in(key, 23)
    wave_axis = jax.random.randint(first_key, (), 3 * MX // 4, MX - 1)
    north_axis = jax.random.randint(second_key, (), 3 * (NY // 2) // 4, NY // 2)
    wave_index = jnp.arange(MX, dtype=jnp.int32)
    north_index = jnp.arange(NY // 2, dtype=jnp.int32)
    scaled = wave_index * north_axis // wave_axis
    inside = north_index[None, :] * north_index[None, :] + scaled[:, None] * scaled[:, None] <= north_axis * north_axis
    counted = jnp.sum(inside.astype(jnp.int32), axis=1) - 1
    shaped = jnp.where(wave_index > wave_axis, -1, counted)
    return jnp.where(wave_index == 0, NY // 2 - 1, shaped).astype(jnp.int32)


def level_of(stream_key, dims, split, low, top_value):
    gain, own = 1.0, jax.random.fold_in(stream_key, 6)
    for axis_at, blocks in split:
        draws = jnp.exp(jax.random.uniform(jax.random.fold_in(own, axis_at), (blocks,), jnp.float32, low / len(split), top_value / len(split)))
        gain = gain * jnp.repeat(draws, dims[axis_at] // blocks).reshape([-1 if axis == axis_at else 1 for axis in range(len(dims))])
    return gain


def centred(rng, dims, deviation, bound, shards=(), kind=jnp.bfloat16):
    gain = level_of(rng, dims, shards, -0.22, 0.18) if shards else 1.0
    drawn = jax.random.normal(rng, dims, jnp.float32) * deviation * gain
    return jnp.minimum(jnp.maximum(drawn, -bound), bound).astype(kind)


def setup_inputs(seed: int = 0) -> dict:
    key_of = jax.random.split(jax.random.key(seed), 5)
    return {
        "vorticity": centred(key_of[0], (2, LEVELS, MX, NY), (0.6 * NX ** -1), 0.0017578125, ((1, 4), (2, 8)), jnp.float32),
        "divergence": centred(key_of[1], (2, LEVELS, MX, NY), (0.6 * NX ** -1), 0.0017578125, ((1, 4), (2, 8)), jnp.float32),
        "trunc_cut": draw_trunc_cut(jax.random.fold_in(key_of[4], 71), 0),
        "level_slot": jax.random.permutation(key_of[3], LEVELS).astype(jnp.int32),
    }


def reference(vorticity, divergence, trunc_cut, level_slot):
    wave_index = jnp.arange(NX // 2, dtype=jnp.int32)
    north_index = jnp.arange(NY, dtype=jnp.int32)
    north_wave = jnp.where(north_index < NY // 2, north_index, north_index - NY)
    wave_east = (2.0 * math.pi / NX) * wave_index.astype(jnp.float32)
    wave_north = (2.0 * math.pi / NY) * north_wave.astype(jnp.float32)
    east_col = wave_east[:, None]
    north_row = wave_north[None, :]
    square_wave = east_col * east_col + north_row * north_row
    retained = (jnp.abs(north_wave)[None, :] <= trunc_cut[:, None]) & (square_wave > 0)
    inverse_square = jnp.where(retained, 1.0 / jnp.where(square_wave > 0, square_wave, 1.0), 0.0)
    weights = jnp.where(wave_index == 0, 1.0, 2.0).astype(jnp.float32)

    def one_level(slot_data):
        curl_real, curl_imag, source_real, source_imag = slot_data
        east_real = (-north_row * curl_imag + east_col * source_imag) * inverse_square
        east_imag = (north_row * curl_real - east_col * source_real) * inverse_square
        north_real = (east_col * curl_imag + north_row * source_imag) * inverse_square
        north_imag = (-east_col * curl_real - north_row * source_real) * inverse_square
        results = []
        for real_part, imag_part in ((east_real, east_imag), (north_real, north_imag)):
            coeffs = real_part + 1j * imag_part
            meridional = jnp.fft.ifft(coeffs, axis=1) * NY
            weighted = meridional * weights[:, None]
            padded = jnp.concatenate([weighted, jnp.zeros_like(weighted)], axis=0)
            value_grid = (jnp.fft.ifft(padded, axis=0) * NX).real.T
            sloped = jnp.concatenate([weighted * (1j * wave_east[:, None]), jnp.zeros_like(weighted)], axis=0)
            slope_grid = (jnp.fft.ifft(sloped, axis=0) * NX).real.T
            results.append(value_grid)
            results.append(slope_grid)
        return tuple(results)

    values = lax.map(one_level, (vorticity[0], vorticity[1], divergence[0], divergence[1]))
    inverse = jnp.argsort(level_slot).astype(jnp.int32)
    return (values[0][inverse], values[2][inverse], values[1][inverse], values[3][inverse])
```

```python
import functools
import math

import jax
import jax.numpy as jnp
import numpy as np
from jax import lax
from jax.experimental import pallas as pl
from jax.experimental.pallas import tpu as pltpu
from jax.sharding import Mesh, PartitionSpec as P


HIGHEST = lax.Precision.HIGHEST
LANES = 128
SUBLANES = 8
EAST_RADIX = 8
ROW_STEP = 16
F32 = jnp.float32
BF16 = jnp.bfloat16
ANY = pl.ANY


def cmul_root(value, k, n):
    re, im = value
    k = k % n
    if k == 0:
        return re, im
    if 4 * k == n:
        return -im, re
    if 2 * k == n:
        return -re, -im
    half = math.sqrt(0.5)
    if 8 * k == n:
        return (re - im) * half, (re + im) * half
    if 8 * k == 3 * n:
        return (re + im) * -half, (re - im) * half
    c = math.cos(2.0 * math.pi * k / n)
    s = math.sin(2.0 * math.pi * k / n)
    return re * c - im * s, re * s + im * c


def small_dft(values):
    n = len(values)
    if n == 1:
        return values
    even = small_dft(values[0::2])
    odd = small_dft(values[1::2])
    low, high = [], []
    for k in range(n // 2):
        er, ei = even[k]
        tr, ti = cmul_root(odd[k], k, n)
        low.append((er + tr, ei + ti))
        high.append((er - tr, ei - ti))
    return low + high


def small_dft_real(values):
    (r0, _), (r1, i1), (r2, i2), (r3, i3), (r4, _), (r5, i5), (r6, i6), (r7, i7) = values
    half = math.sqrt(0.5)
    s0, d0 = r0 + r4, r0 - r4
    s2, d2 = r2 + r6, i2 - i6
    s1r, d1r = r1 + r5, r1 - r5
    s1i, d1i = i1 + i5, i1 - i5
    s3r, d3r = r3 + r7, r3 - r7
    s3i, d3i = i3 + i7, i3 - i7
    p, q = s0 + s2, s1r + s3r
    e, f = s0 - s2, s1i - s3i
    g1r, g1i = (d1r - d1i) * half, (d1r + d1i) * half
    g3r, g3i = (d3r + d3i) * -half, (d3r - d3i) * half
    t, u = d0 - d2, g1r + g3r
    v, w = d0 + d2, g1i - g3i
    return [p + q, t + u, e - f, v - w, p - q, t - u, e + f, v + w]


def split_f32(value):
    high = value.astype(BF16)
    low = (value - high.astype(F32)).astype(BF16)
    return high, low


def north_tables(north_cells, radix, rows_out, devices):
    fast = north_cells // radix
    per_owner = rows_out // radix
    n2 = np.arange(fast)
    y2 = np.arange(devices)[:, None] * per_owner + np.arange(per_owner)[None, :]
    angle = 2.0 * np.pi / fast * ((y2[:, :, None] * n2[None, None, :]) % fast)
    c, s = np.cos(angle), np.sin(angle)
    real_rows = np.concatenate([c, -s], axis=2)
    imag_rows = np.concatenate([s, c], axis=2)
    matrix = np.concatenate([real_rows, imag_rows], axis=1).reshape(2 * fast, 2 * fast)
    matrix = matrix.astype(np.float32)
    high = matrix.astype(BF16)
    low = (matrix - high.astype(np.float32)).astype(BF16)
    turn = 2.0 * np.pi / north_cells * (np.arange(radix)[:, None] * n2[None, :])
    twiddle = np.stack([np.cos(turn), np.sin(turn)]).astype(np.float32)
    return np.stack([high, low]), twiddle


def north_kernel(
    wind, radix, east_cells, north_cells, steps,
    place_ref, cut_ref, vort_ref, div_ref, matrix_ref, twiddle_ref, *rest,
):
    *out_refs, cut_rows, g_high, g_low = rest
    step = pl.program_id(0)
    waves = cut_ref.shape[1]
    fast = north_cells // radix
    block_rows = vort_ref.shape[2]
    east_unit = 2.0 * math.pi / east_cells
    north_unit = 2.0 * math.pi / north_cells

    @pl.when(step == 0)
    def _():
        cut_rows[...] = jnp.broadcast_to(cut_ref[...], (LANES, waves)).T

    lane = lax.broadcasted_iota(jnp.int32, (ROW_STEP, LANES), 1)
    sub = lax.broadcasted_iota(jnp.int32, (ROW_STEP, LANES), 0)
    for part in range(block_rows // ROW_STEP):
        local = part * ROW_STEP
        base = pl.multiple_of(step * block_rows + local, ROW_STEP)
        cut = cut_rows[pl.ds(base, ROW_STEP), :]
        wave = place_ref[0] + base + sub
        kx = east_unit * wave.astype(F32)
        kx2 = kx * kx
        weight = jnp.where(wave == 0, 1.0, 2.0).astype(F32)
        values = []
        for n1 in range(radix):
            cols = slice(n1 * fast, (n1 + 1) * fast)
            index = lane + n1 * fast
            signed = jnp.where(index < north_cells // 2, index, index - north_cells)
            ky = north_unit * signed.astype(F32)
            square = kx2 + ky * ky
            positive = square > 0
            keep = (jnp.abs(signed) <= cut) & positive
            inverse = jnp.where(keep, weight / jnp.where(positive, square, 1.0), 0.0)
            zr = vort_ref[0, 0, local:local + ROW_STEP, cols]
            zi = vort_ref[1, 0, local:local + ROW_STEP, cols]
            dr = div_ref[0, 0, local:local + ROW_STEP, cols]
            di = div_ref[1, 0, local:local + ROW_STEP, cols]
            if wind == 0:
                re, im = kx * di - ky * zi, ky * zr - kx * dr
            else:
                re, im = kx * zi + ky * di, -kx * zr - ky * dr
            values.append((re * inverse, im * inverse))
        result = small_dft(values)
        for y1 in range(radix):
            re, im = result[y1]
            if y1:
                c = twiddle_ref[0, y1:y1 + 1, :]
                s = twiddle_ref[1, y1:y1 + 1, :]
                re, im = re * c - im * s, re * s + im * c
            row = pl.multiple_of(y1 * waves + base, ROW_STEP)
            high, low = split_f32(re)
            g_high[pl.ds(row, ROW_STEP), 0:fast] = high
            g_low[pl.ds(row, ROW_STEP), 0:fast] = low
            high, low = split_f32(im)
            g_high[pl.ds(row, ROW_STEP), fast:2 * fast] = high
            g_low[pl.ds(row, ROW_STEP), fast:2 * fast] = low

    @pl.when(step == steps - 1)
    def _():
        contract = (((1,), (1,)), ((), ()))
        dot = functools.partial(lax.dot_general, dimension_numbers=contract, preferred_element_type=F32)
        height = place_ref[1]
        planes = len(out_refs) if len(out_refs) > 1 else out_refs[0].shape[1]
        owners = out_refs[0].shape[0]
        span = owners * SUBLANES

        def rows_of(kind):
            return jnp.concatenate(
                [matrix_ref[kind, pl.ds((height ^ j) * span, span), :] for j in range(planes)], axis=0
            )

        matrix_high, matrix_low = rows_of(0), rows_of(1)
        for pair in range(radix // 2):
            rows = slice(pair * 2 * waves, (pair + 1) * 2 * waves)
            high = g_high[rows, :]
            low = g_low[rows, :]
            product = dot(matrix_high, high) + dot(matrix_high, low) + dot(matrix_low, high)
            for part in range(2):
                y1 = 2 * pair + part
                for j in range(planes):
                    piece = product[j * span:(j + 1) * span, part * waves:(part + 1) * waves]
                    piece = piece.reshape(owners, SUBLANES, waves)
                    if len(out_refs) > 1:
                        out_refs[j][:, y1] = piece
                    else:
                        out_refs[0][:, j, y1] = piece


def north_call(place, cut, vort, div, matrix, twiddle, slot, wind, radix, east_cells, planes, owners, apart):
    waves = vort.shape[2]
    north_cells = vort.shape[3]
    steps = 4
    block_rows = waves // steps
    fast = north_cells // radix
    data_spec = pl.BlockSpec((2, 1, block_rows, north_cells), lambda i: (0, slot, i, 0))
    kernel = functools.partial(north_kernel, wind, radix, east_cells, north_cells, steps)
    flops = 6 * (2 * fast) ** 2 * radix * waves
    tile = (radix, SUBLANES, waves)
    shape = (owners,) + tile if apart else (owners, planes) + tile
    whole = pl.BlockSpec(shape, lambda i: (0,) * len(shape))
    out_specs = [whole] * (planes if apart else 1)
    return pl.pallas_call(
        kernel,
        grid=(steps,),
        in_specs=[
            pl.BlockSpec(memory_space=pltpu.SMEM),
            pl.BlockSpec((1, waves), lambda i: (0, 0)),
            data_spec,
            data_spec,
            pl.BlockSpec(matrix.shape, lambda i: (0, 0, 0)),
            pl.BlockSpec(twiddle.shape, lambda i: (0, 0, 0)),
        ],
        out_specs=out_specs,
        out_shape=[jax.ShapeDtypeStruct(shape, F32)] * len(out_specs),
        scratch_shapes=[
            pltpu.VMEM((waves, LANES), jnp.int32),
            pltpu.VMEM((radix * waves, 2 * fast), BF16),
            pltpu.VMEM((radix * waves, 2 * fast), BF16),
        ],
        compiler_params=pltpu.CompilerParams(dimension_semantics=("arbitrary",)),
        cost_estimate=pl.CostEstimate(flops=flops, bytes_accessed=6 << 20, transcendentals=0),
    )(place, cut, vort, div, matrix, twiddle)


def east_tables(columns, local_waves, east_cells, height, width):
    radix = EAST_RADIX
    span = east_cells // radix
    lane = jnp.arange(LANES, dtype=jnp.int32)
    column = (lane % columns) ^ (height * width)
    base = column * local_waves + (lane // columns) * radix
    wave = jnp.arange(radix, dtype=jnp.int32)[:, None] + base[None, :]
    steps = wave[:, :, None] * jnp.arange(span, dtype=jnp.int32)[None, None, :] % east_cells
    angle = 2.0 * math.pi / east_cells * steps.astype(F32)
    kx = (2.0 * math.pi / east_cells * wave.astype(F32))[:, :, None]
    c, s = jnp.cos(angle), jnp.sin(angle)
    kc, ks = kx * c, kx * s
    real_rows = jnp.concatenate([c, s, -ks, kc], axis=2)
    imag_rows = jnp.concatenate([-s, c, -kc, -ks], axis=2)
    table = jnp.concatenate([real_rows, imag_rows], axis=1)
    high = lax.reduce_precision(table, 8, 7)
    low = (table - high).astype(BF16)
    return high.astype(BF16), low


def east_kernel(slot, slots_local, planes, *refs):
    level_ref, high_ref, low_ref = refs[:3]
    got_refs = refs[3:3 + planes]
    value_ref, slope_ref, h_high, h_low, spectra, grid_out, sems = refs[-7:]
    step = pl.program_id(0)
    radix = EAST_RADIX
    width, groups, packed, lanes = got_refs[0].shape
    columns = planes * width
    north_radix = packed // SUBLANES
    per_owner = SUBLANES // 2
    rows_out = north_radix * per_owner
    span = spectra.shape[2] // 4

    @pl.when(step == 0)
    def _():
        lane = lax.broadcasted_iota(jnp.int32, (north_radix, lanes), 1)

        def shuffle(group, carry):
            for y2 in range(per_owner):
                for ri in range(2):
                    slabs = [
                        got_refs[c // width][c % width, group, pl.ds(ri * per_owner + y2, north_radix, stride=SUBLANES), :]
                        for c in range(columns)
                    ]
                    bit = 1
                    while bit < columns:
                        mask = (lane & bit) == 0
                        for c in range(columns):
                            if c & bit == 0:
                                a, b = slabs[c], slabs[c | bit]
                                slabs[c] = jnp.where(mask, a, pltpu.roll(b, bit, 1))
                                slabs[c | bit] = jnp.where(mask, pltpu.roll(a, lanes - bit, 1), b)
                        bit *= 2
                    row = pl.multiple_of(group * rows_out + y2 * north_radix, north_radix)
                    for a in range(radix):
                        high, low = split_f32(slabs[a])
                        h_high[a, pl.ds(row, north_radix), ri * lanes:(ri + 1) * lanes] = high
                        h_low[a, pl.ds(row, north_radix), ri * lanes:(ri + 1) * lanes] = low
            return carry

        lax.fori_loop(0, groups, shuffle, 0)

    dot = functools.partial(jnp.dot, preferred_element_type=F32)
    left, left_low = h_high[step], h_low[step]
    spectra[step] = dot(left, high_ref[0]) + dot(left_low, high_ref[0]) + dot(left, low_ref[0])

    @pl.when(step == radix - 1)
    def _():
        copies = []
        for group in range(groups):
            level = level_ref[group * slots_local + slot]
            for kind in range(2):

                def combine(block, carry, group=group, kind=kind):
                    row = pl.multiple_of(group * rows_out + block * SUBLANES, SUBLANES)
                    for tile in range(span // LANES):
                        first = 2 * kind * span + tile * LANES
                        values = [
                            (
                                spectra[a, pl.ds(row, SUBLANES), first:first + LANES],
                                spectra[a, pl.ds(row, SUBLANES), first + span:first + span + LANES],
                            )
                            for a in range(radix)
                        ]
                        outs = small_dft_real(values)
                        for x1 in range(radix):
                            at = x1 * span + tile * LANES
                            grid_out[kind, pl.ds(row, SUBLANES), at:at + LANES] = outs[x1]
                    return carry

                lax.fori_loop(0, rows_out // SUBLANES, combine, 0, unroll=2)
                target = value_ref if kind == 0 else slope_ref
                copy = pltpu.make_async_copy(
                    grid_out.at[kind, pl.ds(group * rows_out, rows_out), :],
                    target.at[level],
                    sems.at[2 * group + kind],
                )
                copy.start()
                copies.append(copy)
        for copy in copies:
            copy.wait()


def east_call(levels, got, high, low, slot, slots_local, east_cells, previous):
    planes = len(got)
    width, groups, packed, lanes = got[0][0].shape[0], got[0][0].shape[1], *got[0][0].shape[-2:]
    rows_out = packed // 2
    radix = EAST_RADIX
    level_count = levels.shape[0]
    out = jax.ShapeDtypeStruct((level_count, rows_out, east_cells), F32)
    in_specs = [
        pl.BlockSpec(memory_space=pltpu.SMEM),
        pl.BlockSpec((1,) + high.shape[1:], lambda i: (i, 0, 0)),
        pl.BlockSpec((1,) + low.shape[1:], lambda i: (i, 0, 0)),
    ]
    operands = [levels, high, low]
    for array, plane in got:
        if plane is None:
            in_specs.append(pl.BlockSpec(array.shape, lambda i: (0, 0, 0, 0)))
        else:
            in_specs.append(
                pl.BlockSpec((width, groups, None, packed, lanes), lambda i, plane=plane: (0, 0, plane, 0, 0))
            )
        operands.append(array)
    aliases = {}
    if previous is not None:
        aliases = {len(operands): 0, len(operands) + 1: 1}
        in_specs += [pl.BlockSpec(memory_space=ANY)] * 2
        operands += list(previous)
    rows = groups * rows_out
    return pl.pallas_call(
        functools.partial(east_kernel, slot, slots_local, planes),
        grid=(radix,),
        in_specs=in_specs,
        out_specs=[pl.BlockSpec(memory_space=ANY)] * 2,
        out_shape=[out, out],
        scratch_shapes=[
            pltpu.VMEM((radix, rows, 2 * lanes), BF16),
            pltpu.VMEM((radix, rows, 2 * lanes), BF16),
            pltpu.VMEM((radix, rows, high.shape[2]), F32),
            pltpu.VMEM((2, rows, east_cells), F32),
            pltpu.SemaphoreType.DMA((2 * groups,)),
        ],
        input_output_aliases=aliases,
        compiler_params=pltpu.CompilerParams(dimension_semantics=("arbitrary",)),
        cost_estimate=pl.CostEstimate(
            flops=6 * radix * rows * high.shape[1] * high.shape[2], bytes_accessed=14 << 20, transcendentals=0
        ),
    )(*operands)


def fast_shapes(mesh, vorticity):
    columns = mesh.shape["height"] * mesh.shape["width"]
    groups = mesh.shape["row"]
    waves = vorticity.shape[2]
    north_cells = vorticity.shape[3]
    rows_out = north_cells // (columns * groups)
    radix = rows_out // (SUBLANES // 2)
    return (
        waves == LANES
        and columns == EAST_RADIX
        and radix >= 2
        and radix & (radix - 1) == 0
        and north_cells == radix * LANES
    )


def fast_on_device(*args):
    return fast_body(*args)


def fast_body(vorticity, divergence, trunc_cut, level_slot):
    planes = lax.axis_size("height")
    width = lax.axis_size("width")
    groups = lax.axis_size("row")
    columns = planes * width
    slots_local = vorticity.shape[1]
    waves = vorticity.shape[2]
    north_cells = vorticity.shape[3]
    east_cells = 2 * waves * columns
    rows_out = north_cells // (columns * groups)
    radix = rows_out // (SUBLANES // 2)
    height = lax.axis_index("height").astype(jnp.int32)
    column = height * width + lax.axis_index("width")
    place = jnp.stack([column * waves, height]).astype(jnp.int32)
    matrix, twiddle = north_tables(north_cells, radix, rows_out, columns * groups)
    cut = trunc_cut.reshape(1, waves)
    packed = radix * SUBLANES
    swaps = [[(z, z ^ j) for z in range(planes)] for j in range(planes)]
    order = list(range(planes - 1, 0, -1))

    def north(slot, wind, apart):
        return north_call(
            place, cut, vorticity, divergence, matrix, twiddle, slot, wind, radix, east_cells,
            planes, width * groups, apart,
        )

    def swap(parts):
        got = {0: parts[0]}
        for j in order:
            got[j] = lax.ppermute(parts[j], "height", swaps[j])
        return got

    def around(block):
        return lax.all_to_all(block, ("width", "row"), split_axis=0, concat_axis=0, tiled=True)

    chunks = [(slot, wind) for slot in range(slots_local) for wind in range(2)]
    high, low = east_tables(columns, waves, east_cells, height, width)
    outputs = [None, None]
    ready = []
    for at, (slot, wind) in enumerate(chunks):
        if at == 0:
            swapped = swap(north(slot, wind, True))
            block = jnp.stack([swapped[j] for j in range(planes)], axis=1)
            block = around(block).reshape(width, groups, planes, packed, waves)
            ready.append([(block, j) for j in range(planes)])
        else:
            block = around(north(slot, wind, False)[0])
            swapped = swap([block[:, j] for j in range(planes)])
            ready.append([(swapped[j].reshape(width, groups, packed, waves), None) for j in range(planes)])
    for at in [1, 0] + list(range(2, len(chunks))):
        slot, wind = chunks[at]
        outputs[wind] = east_call(
            level_slot, ready[at], high, low, slot, slots_local, east_cells, outputs[wind]
        )
    return (outputs[0][0], outputs[1][0], outputs[0][1], outputs[1][1])


def spectral_winds(vorticity, divergence, trunc_cut, first_wave, east_cells):
    local_count = vorticity.shape[2]
    north_cells = vorticity.shape[3]
    wave_index = first_wave + jnp.arange(local_count, dtype=jnp.int32)
    north_index = jnp.arange(north_cells, dtype=jnp.int32)
    north_wave = jnp.where(north_index < north_cells // 2, north_index, north_index - north_cells)
    wave_east = 2.0 * math.pi / east_cells * wave_index.astype(jnp.float32)
    wave_north = 2.0 * math.pi / north_cells * north_wave.astype(jnp.float32)
    east_col = wave_east[:, None]
    north_row = wave_north[None, :]
    square_wave = east_col * east_col + north_row * north_row
    retained = (jnp.abs(north_wave)[None, :] <= trunc_cut[:, None]) & (square_wave > 0)
    inverse_square = jnp.where(retained, 1.0 / jnp.where(square_wave > 0, square_wave, 1.0), 0.0)
    curl_real = vorticity[0]
    curl_imag = vorticity[1]
    source_real = divergence[0]
    source_imag = divergence[1]
    east_real = (-north_row * curl_imag + east_col * source_imag) * inverse_square
    east_imag = (north_row * curl_real - east_col * source_real) * inverse_square
    north_real = (east_col * curl_imag + north_row * source_imag) * inverse_square
    north_imag = (-east_col * curl_real - north_row * source_real) * inverse_square
    return jnp.stack([east_real, east_imag, north_real, north_imag], axis=1)


def north_transform(flattened, local_waves):
    slot_count = flattened.shape[0]
    north_cells = flattened.shape[2]
    block_size = math.gcd(north_cells, 256)
    block_count = north_cells // block_size
    north_index = jnp.arange(north_cells, dtype=jnp.int32)

    def north_one_block(block_index, result):
        row_index = block_index * block_size + jnp.arange(block_size, dtype=jnp.int32)
        phase_steps = row_index[:, None] * north_index[None, :] % north_cells
        angles = 2.0 * math.pi / north_cells * phase_steps.astype(jnp.float32)
        cosine_table = jnp.cos(angles)
        sine_table = jnp.sin(angles)
        with_cosine = jnp.einsum("yn,lkn->lyk", cosine_table, flattened, precision=HIGHEST)
        with_sine = jnp.einsum("yn,lkn->lyk", sine_table, flattened, precision=HIGHEST)
        with_cosine = with_cosine.reshape(slot_count, block_size, 2, 2, local_waves)
        with_sine = with_sine.reshape(slot_count, block_size, 2, 2, local_waves)
        real_part = with_cosine[:, :, :, 0] - with_sine[:, :, :, 1]
        imag_part = with_sine[:, :, :, 0] + with_cosine[:, :, :, 1]
        joined = jnp.concatenate([real_part, imag_part], axis=3)
        return lax.dynamic_update_slice_in_dim(result, joined, block_index * block_size, 1)

    initial = jnp.zeros((slot_count, north_cells, 2, 2 * local_waves), jnp.float32)
    return lax.fori_loop(0, block_count, north_one_block, initial)


def east_transform(stacked, local_waves, east_cells):
    columns = stacked.shape[0]
    slot_count = stacked.shape[1]
    row_count = stacked.shape[2]
    field_count = stacked.shape[3]
    block_size = math.gcd(east_cells, 256)
    block_count = east_cells // block_size
    wave_number = (
        jnp.arange(columns, dtype=jnp.int32)[:, None] * local_waves
        + jnp.arange(local_waves, dtype=jnp.int32)[None, :]
    )
    weights = jnp.where(wave_number == 0, 1.0, 2.0)[:, :, None]
    wave_east = 2.0 * math.pi / east_cells * wave_number.astype(jnp.float32)[:, :, None]

    def east_one_block(block_index, result):
        east_index = block_index * block_size + jnp.arange(block_size, dtype=jnp.int32)
        phase_steps = wave_number[:, :, None] * east_index[None, None, :] % east_cells
        angles = 2.0 * math.pi / east_cells * phase_steps.astype(jnp.float32)
        cosine_table = jnp.cos(angles)
        sine_table = jnp.sin(angles)
        value_real = weights * cosine_table
        value_imag = -weights * sine_table
        slope_real = -weights * wave_east * sine_table
        slope_imag = -weights * wave_east * cosine_table
        value_table = jnp.stack([value_real, value_imag], axis=1)
        slope_table = jnp.stack([slope_real, slope_imag], axis=1)
        east_table = jnp.stack([value_table, slope_table], axis=3).reshape(
            columns, 2 * local_waves, 2, block_size
        )
        product = jnp.einsum("clyfk,ckab->falyb", stacked, east_table, precision=HIGHEST)
        return lax.dynamic_update_slice_in_dim(result, product, block_index * block_size, 4)

    initial = jnp.zeros((field_count, 2, slot_count, row_count, east_cells), jnp.float32)
    return lax.fori_loop(0, block_count, east_one_block, initial)


def place_levels(grid_all, level_slot):
    slot_count = grid_all.shape[2]
    selector = (level_slot[None, :] == jnp.arange(slot_count, dtype=jnp.int32)[:, None]).astype(
        jnp.float32
    )
    return jnp.einsum("ls,fasyx->falyx", selector, grid_all, precision=HIGHEST)


def plain_on_device(vorticity, divergence, trunc_cut, level_slot):
    columns = lax.axis_size("col")
    row_count = lax.axis_size("row")
    local_waves = vorticity.shape[2]
    north_cells = vorticity.shape[3]
    east_cells = 2 * local_waves * columns
    first_wave = lax.axis_index("col") * local_waves
    spectra = spectral_winds(vorticity, divergence, trunc_cut, first_wave, east_cells)
    slot_count = spectra.shape[0]
    flattened = spectra.reshape(slot_count, 4 * local_waves, north_cells)
    fourier = north_transform(flattened, local_waves)
    outgoing = fourier[None]
    received = lax.all_to_all(outgoing, ("col", "row"), split_axis=2, concat_axis=0, tiled=True)
    shaped = received.reshape(
        columns,
        row_count * received.shape[1],
        received.shape[2],
        received.shape[3],
        received.shape[4],
    )
    grid_all = east_transform(shaped, local_waves, east_cells)
    placed = place_levels(grid_all, level_slot)
    return (placed[0, 0], placed[1, 0], placed[0, 1], placed[1, 1])


def solution(mesh):
    columns = mesh.shape["col"]
    groups = mesh.shape["row"]
    width = 2 if columns % 2 == 0 else 1
    fine = Mesh(mesh.devices.reshape(columns // width, width, groups), ("height", "width", "row"))

    def whole(vorticity, divergence, trunc_cut, level_slot):
        waves = vorticity.shape[2] // columns
        local = jax.ShapeDtypeStruct((2, vorticity.shape[1] // groups, waves, vorticity.shape[3]), F32)
        fast = fast_shapes(fine, local)
        column = ("height", "width") if fast else "col"
        grid = P(None, ("height", "width", "row") if fast else ("col", "row"), None)
        spectral = P(None, "row", column, None)
        return jax.shard_map(
            fast_on_device if fast else plain_on_device,
            mesh=fine if fast else mesh,
            in_specs=(spectral, spectral, P(column), P()),
            out_specs=(grid, grid, grid, grid),
            check_vma=False,
        )(vorticity, divergence, trunc_cut, level_slot)

    return whole
```

```python
import functools
import math

import jax
import jax.numpy as jnp
import numpy as np
from jax import lax
from jax.experimental import pallas as pl
from jax.experimental.pallas import tpu as pltpu
from jax.sharding import Mesh, PartitionSpec as P


HIGHEST = lax.Precision.HIGHEST
LANES = 128
SUBLANES = 8
EAST_RADIX = 8
CHUNKS = 4
LAST_PIECES = 2
F32 = jnp.float32
BF16 = jnp.bfloat16
ANY = pl.ANY


def cmul_root(value, k, n):
    re, im = value
    k = k % n
    if k == 0:
        return re, im
    if 4 * k == n:
        return -im, re
    if 2 * k == n:
        return -re, -im
    half = math.sqrt(0.5)
    if 8 * k == n:
        return (re - im) * half, (re + im) * half
    if 8 * k == 3 * n:
        return (re + im) * -half, (re - im) * half
    c = math.cos(2.0 * math.pi * k / n)
    s = math.sin(2.0 * math.pi * k / n)
    return re * c - im * s, re * s + im * c


def small_dft(values):
    n = len(values)
    if n == 1:
        return values
    even = small_dft(values[0::2])
    odd = small_dft(values[1::2])
    low, high = [], []
    for k in range(n // 2):
        er, ei = even[k]
        tr, ti = cmul_root(odd[k], k, n)
        low.append((er + tr, ei + ti))
        high.append((er - tr, ei - ti))
    return low + high


def small_dft_real(values):
    (r0, _), (r1, i1), (r2, i2), (r3, i3), (r4, _), (r5, i5), (r6, i6), (r7, i7) = values
    half = math.sqrt(0.5)
    s0, d0 = r0 + r4, r0 - r4
    s2, d2 = r2 + r6, i2 - i6
    s1r, d1r = r1 + r5, r1 - r5
    s1i, d1i = i1 + i5, i1 - i5
    s3r, d3r = r3 + r7, r3 - r7
    s3i, d3i = i3 + i7, i3 - i7
    p, q = s0 + s2, s1r + s3r
    e, f = s0 - s2, s1i - s3i
    g1r, g1i = (d1r - d1i) * half, (d1r + d1i) * half
    g3r, g3i = (d3r + d3i) * -half, (d3r - d3i) * half
    t, u = d0 - d2, g1r + g3r
    v, w = d0 + d2, g1i - g3i
    return [p + q, t + u, e - f, v - w, p - q, t - u, e + f, v + w]


def split_f32(value):
    high = value.astype(BF16)
    low = (value - high.astype(F32)).astype(BF16)
    return high, low


def north_tables(north_cells, radix, rows_out, devices):
    fast = north_cells // radix
    per_owner = rows_out // radix
    n2 = np.arange(fast)
    y2 = np.arange(devices)[:, None] * per_owner + np.arange(per_owner)[None, :]
    angle = 2.0 * np.pi / fast * ((y2[:, :, None] * n2[None, None, :]) % fast)
    c, s = np.cos(angle), np.sin(angle)
    real_rows = np.concatenate([c, -s], axis=2)
    imag_rows = np.concatenate([s, c], axis=2)
    matrix = np.concatenate([real_rows, imag_rows], axis=1).reshape(2 * fast, 2 * fast)
    matrix = matrix.astype(np.float32)
    high = matrix.astype(BF16)
    low = (matrix - high.astype(np.float32)).astype(BF16)
    turn = 2.0 * np.pi / north_cells * (np.arange(radix)[:, None] * n2[None, :])
    twiddle = np.stack([np.cos(turn), np.sin(turn)]).astype(np.float32)
    return np.stack([high, low]), twiddle


def north_kernel(
    wind, radix, east_cells, north_cells, steps,
    place_ref, cut_ref, vort_ref, div_ref, matrix_ref, twiddle_ref, *rest,
):
    *out_refs, cut_rows, winds, g_high, g_low = rest
    step = pl.program_id(0)
    waves = cut_ref.shape[1]
    fast = north_cells // radix
    block_rows = vort_ref.shape[2]
    east_unit = 2.0 * math.pi / east_cells
    north_unit = 2.0 * math.pi / north_cells

    @pl.when(step == 0)
    def _():
        cut_rows[...] = jnp.broadcast_to(cut_ref[...], (LANES, waves)).T

    lane = lax.broadcasted_iota(jnp.int32, (SUBLANES, LANES), 1)
    sub = lax.broadcasted_iota(jnp.int32, (SUBLANES, LANES), 0)

    def wind_rows(part, carry):
        local = pl.multiple_of(part * SUBLANES, SUBLANES)
        base = pl.multiple_of(step * block_rows + local, SUBLANES)
        cut = cut_rows[pl.ds(base, SUBLANES), :]
        wave = place_ref[0] + base + sub
        kx = east_unit * wave.astype(F32)
        kx2 = kx * kx
        weight = jnp.where(wave == 0, 1.0, 2.0).astype(F32)
        for n1 in range(radix):
            cols = slice(n1 * fast, (n1 + 1) * fast)
            index = lane + n1 * fast
            signed = jnp.where(index < north_cells // 2, index, index - north_cells)
            ky = north_unit * signed.astype(F32)
            square = kx2 + ky * ky
            positive = square > 0
            keep = (jnp.abs(signed) <= cut) & positive
            inverse = jnp.where(keep, weight / jnp.where(positive, square, 1.0), 0.0)
            zr = vort_ref[0, 0, pl.ds(local, SUBLANES), cols]
            zi = vort_ref[1, 0, pl.ds(local, SUBLANES), cols]
            dr = div_ref[0, 0, pl.ds(local, SUBLANES), cols]
            di = div_ref[1, 0, pl.ds(local, SUBLANES), cols]
            if wind == 0:
                re, im = kx * di - ky * zi, ky * zr - kx * dr
            else:
                re, im = kx * zi + ky * di, -kx * zr - ky * dr
            winds[0, n1, pl.ds(base, SUBLANES), :] = re * inverse
            winds[1, n1, pl.ds(base, SUBLANES), :] = im * inverse
        return carry

    lax.fori_loop(0, block_rows // SUBLANES, wind_rows, 0)

    @pl.when(step == steps - 1)
    def _():
        column = place_ref[2]
        stride = EAST_RADIX
        count = waves // stride

        def transform(t, carry):
            residue = t ^ column
            values = []
            for n1 in range(radix):
                values.append(
                    tuple(winds[ri, n1, pl.ds(residue, count, stride=stride), :] for ri in range(2))
                )
            result = small_dft(values)
            for y1 in range(radix):
                re, im = result[y1]
                if y1:
                    c = twiddle_ref[0, y1:y1 + 1, :]
                    s = twiddle_ref[1, y1:y1 + 1, :]
                    re, im = re * c - im * s, re * s + im * c
                row = pl.multiple_of(y1 * waves + t * count, count)
                high, low = split_f32(re)
                g_high[pl.ds(row, count), 0:fast] = high
                g_low[pl.ds(row, count), 0:fast] = low
                high, low = split_f32(im)
                g_high[pl.ds(row, count), fast:2 * fast] = high
                g_low[pl.ds(row, count), fast:2 * fast] = low
            return carry

        lax.fori_loop(0, stride, transform, 0)

    @pl.when(step == steps - 1)
    def _():
        contract = (((1,), (1,)), ((), ()))
        dot = functools.partial(lax.dot_general, dimension_numbers=contract, preferred_element_type=F32)
        height = place_ref[1]
        planes = len(out_refs) if len(out_refs) > 1 else out_refs[0].shape[1]
        owners = out_refs[0].shape[0]
        span = owners * SUBLANES

        def rows_of(kind):
            return jnp.concatenate(
                [matrix_ref[kind, pl.ds((height ^ j) * span, span), :] for j in range(planes)], axis=0
            )

        matrix_high, matrix_low = rows_of(0), rows_of(1)
        for pair in range(radix // 2):
            rows = slice(pair * 2 * waves, (pair + 1) * 2 * waves)
            high = g_high[rows, :]
            low = g_low[rows, :]
            product = dot(matrix_high, high) + dot(matrix_high, low) + dot(matrix_low, high)
            for part in range(2):
                y1 = 2 * pair + part
                for j in range(planes):
                    piece = product[j * span:(j + 1) * span, part * waves:(part + 1) * waves]
                    piece = piece.reshape(owners, SUBLANES, waves)
                    if len(out_refs) > 1:
                        out_refs[j][:, y1] = piece
                    else:
                        out_refs[0][:, j, y1] = piece


def north_call(place, cut, vort, div, matrix, twiddle, slot, wind, radix, east_cells, planes, owners, apart):
    waves = vort.shape[2]
    north_cells = vort.shape[3]
    steps = 2
    block_rows = waves // steps
    fast = north_cells // radix
    data_spec = pl.BlockSpec((2, 1, block_rows, north_cells), lambda i: (0, slot, i, 0))
    kernel = functools.partial(north_kernel, wind, radix, east_cells, north_cells, steps)
    flops = 6 * (2 * fast) ** 2 * radix * waves
    tile = (radix, SUBLANES, waves)
    shape = (owners,) + tile if apart else (owners, planes) + tile
    whole = pl.BlockSpec(shape, lambda i: (0,) * len(shape))
    out_specs = [whole] * (planes if apart else 1)
    return pl.pallas_call(
        kernel,
        grid=(steps,),
        in_specs=[
            pl.BlockSpec(memory_space=pltpu.SMEM),
            pl.BlockSpec((1, waves), lambda i: (0, 0)),
            data_spec,
            data_spec,
            pl.BlockSpec(matrix.shape, lambda i: (0, 0, 0)),
            pl.BlockSpec(twiddle.shape, lambda i: (0, 0, 0)),
        ],
        out_specs=out_specs,
        out_shape=[jax.ShapeDtypeStruct(shape, F32)] * len(out_specs),
        scratch_shapes=[
            pltpu.VMEM((waves, LANES), jnp.int32),
            pltpu.VMEM((2, radix, waves, fast), F32),
            pltpu.VMEM((radix * waves, 2 * fast), BF16),
            pltpu.VMEM((radix * waves, 2 * fast), BF16),
        ],
        compiler_params=pltpu.CompilerParams(dimension_semantics=("arbitrary",)),
        cost_estimate=pl.CostEstimate(flops=flops, bytes_accessed=6 << 20, transcendentals=0),
    )(place, cut, vort, div, matrix, twiddle)


def east_table(local_waves, east_cells):
    radix = EAST_RADIX
    span = east_cells // radix
    count = LANES // radix
    lane = jnp.arange(LANES, dtype=jnp.int32)[None, :]
    residue = jnp.arange(radix, dtype=jnp.int32)[:, None]
    wave = ((lane // count) ^ residue) * local_waves + (lane % count) * radix + residue
    steps = wave[:, :, None] * jnp.arange(span, dtype=jnp.int32)[None, None, :] % east_cells
    angle = 2.0 * math.pi / east_cells * steps.astype(F32)

    def parts(x):
        high = lax.reduce_precision(x, 8, 7)
        return jnp.stack([high.astype(BF16), (x - high).astype(BF16)], axis=1)

    c, s = parts(jnp.cos(angle)), parts(jnp.sin(angle))
    rows = [jnp.concatenate([c, s], axis=3), jnp.concatenate([-s, c], axis=3)]
    return jnp.concatenate(rows, axis=2)


def east_kernel(slot, slots_local, sources, first_group, east_cells, local_waves, *refs):
    planes = len(sources)
    place_ref, level_ref, table_hbm = refs[:3]
    got_hbm = refs[3:3 + planes]
    value_ref, slope_ref, got, table, h_high, h_low, spectra, grid_out, got_sems, table_sems, out_sems = refs[-11:]
    radix = EAST_RADIX
    _, width, groups, packed, lanes = got.shape
    columns = planes * width
    north_radix = packed // SUBLANES
    per_owner = SUBLANES // 2
    rows_out = north_radix * per_owner
    span = spectra.shape[3] // 2
    height = place_ref[1]

    loads = []
    for j, plane in enumerate(sources):
        source = got_hbm[j]
        if plane is not None:
            source = source.at[:, pl.ds(first_group, groups), plane]
        copy = pltpu.make_async_copy(source, got.at[height ^ j], got_sems.at[j])
        copy.start()
        loads.append(copy)

    def columns_of(a):
        return slice(0, span if a % (radix // 2) == 0 else 2 * span)

    tables = []
    for a in range(radix):
        cols = columns_of(a)
        copy = pltpu.make_async_copy(
            table_hbm.at[a, :, :, cols], table.at[a, :, :, cols], table_sems.at[a]
        )
        copy.start()
        tables.append(copy)
    for copy in loads:
        copy.wait()

    lane = lax.broadcasted_iota(jnp.int32, (north_radix, lanes), 1)
    count = lanes // radix
    group_of = lane // count
    east_unit = 2.0 * math.pi / east_cells
    kx = [
        east_unit * ((group_of ^ a) * local_waves + (lane % count) * radix + a).astype(F32) for a in range(radix)
    ]

    def shuffle(group, carry):
        for y2 in range(per_owner):
            for ri in range(2):
                slabs = [
                    got[c // width, c % width, group, pl.ds(ri * per_owner + y2, north_radix, stride=SUBLANES), :]
                    for c in range(columns)
                ]
                bit = 1
                while bit < columns:
                    mask = (group_of & bit) == 0
                    slabs = [jnp.where(mask, slabs[i], slabs[i ^ bit]) for i in range(columns)]
                    bit *= 2
                row = pl.multiple_of(group * rows_out + y2 * north_radix, north_radix)
                for a in range(radix):
                    sloped = slabs[a] * kx[a]
                    for kind, value, part in ((0, slabs[a], ri), (1, -sloped if ri else sloped, 1 - ri)):
                        high, low = split_f32(value)
                        h_high[kind, a, pl.ds(row, north_radix), part * lanes:(part + 1) * lanes] = high
                        h_low[kind, a, pl.ds(row, north_radix), part * lanes:(part + 1) * lanes] = low
        return carry

    lax.fori_loop(0, groups, shuffle, 0)

    dot = functools.partial(jnp.dot, preferred_element_type=F32)

    def multiply(kind, a):
        cols = columns_of(a)
        left, left_low = h_high[kind, a], h_low[kind, a]
        right, right_low = table[a, 0, :, cols], table[a, 1, :, cols]
        spectra[kind, a, :, cols] = dot(left, right) + dot(left_low, right) + dot(left, right_low)

    def combine(kind, row):
        for tile in range(span // LANES):
            first = tile * LANES
            values = []
            for a in range(radix):
                re = spectra[kind, a, row:row + SUBLANES, first:first + LANES]
                im = None
                if a % (radix // 2):
                    im = spectra[kind, a, row:row + SUBLANES, first + span:first + span + LANES]
                values.append((re, im))
            outs = small_dft_real(values)
            for x1 in range(radix):
                at = x1 * span + first
                grid_out[kind, row:row + SUBLANES, at:at + LANES] = outs[x1]

    def finish(kind, group):
        for row in range(group * rows_out, (group + 1) * rows_out, SUBLANES):
            combine(kind, row)
        level = level_ref[(first_group + group) * slots_local + slot]
        copy = pltpu.make_async_copy(
            grid_out.at[kind, pl.ds(group * rows_out, rows_out), :],
            (value_ref, slope_ref)[kind].at[level],
            out_sems.at[2 * group + kind],
        )
        copy.start()
        return copy

    for copy in tables:
        copy.wait()
    for a in range(radix):
        multiply(0, a)
    copies = []
    share = radix // groups
    for group in range(groups):
        for a in range(group * share, (group + 1) * share):
            multiply(1, a)
        copies.append(finish(0, group))
    for group in range(groups):
        copies.append(finish(1, group))
    for copy in copies:
        copy.wait()


def east_call(
    place, levels, got, table, slot, slots_local, first_group, groups, width, east_cells, local_waves, previous
):
    planes = len(got)
    packed, lanes = got[0][0].shape[-2:]
    rows_out = packed // 2
    radix = EAST_RADIX
    level_count = levels.shape[0]
    out = jax.ShapeDtypeStruct((level_count, rows_out, east_cells), F32)
    in_specs = [pl.BlockSpec(memory_space=pltpu.SMEM)] * 2 + [pl.BlockSpec(memory_space=ANY)] * (1 + planes)
    operands = [place, levels, table] + [array for array, _ in got]
    aliases = {}
    if previous is not None:
        aliases = {len(operands): 0, len(operands) + 1: 1}
        in_specs += [pl.BlockSpec(memory_space=ANY)] * 2
        operands += list(previous)
    rows = groups * rows_out
    columns = table.shape[-1]
    sources = tuple(plane for _, plane in got)
    return pl.pallas_call(
        functools.partial(east_kernel, slot, slots_local, sources, first_group, east_cells, local_waves),
        in_specs=in_specs,
        out_specs=[pl.BlockSpec(memory_space=ANY)] * 2,
        out_shape=[out, out],
        scratch_shapes=[
            pltpu.VMEM((planes, width, groups, packed, lanes), F32),
            pltpu.VMEM(table.shape, BF16),
            pltpu.VMEM((2, radix, rows, 2 * lanes), BF16),
            pltpu.VMEM((2, radix, rows, 2 * lanes), BF16),
            pltpu.VMEM((2, radix, rows, columns), F32),
            pltpu.VMEM((2, rows, east_cells), F32),
            pltpu.SemaphoreType.DMA((planes,)),
            pltpu.SemaphoreType.DMA((radix,)),
            pltpu.SemaphoreType.DMA((2 * groups,)),
        ],
        input_output_aliases=aliases,
        cost_estimate=pl.CostEstimate(
            flops=12 * radix * rows * 2 * lanes * columns, bytes_accessed=14 << 20, transcendentals=0
        ),
    )(*operands)


def fast_shapes(mesh, vorticity):
    columns = mesh.shape["height"] * mesh.shape["width"]
    groups = mesh.shape["row"]
    waves = vorticity.shape[2]
    north_cells = vorticity.shape[3]
    rows_out = north_cells // (columns * groups)
    radix = rows_out // (SUBLANES // 2)
    return (
        waves == LANES
        and columns == EAST_RADIX
        and radix >= 2
        and radix & (radix - 1) == 0
        and north_cells == radix * LANES
        and groups % LAST_PIECES == 0
        and EAST_RADIX % groups == 0
        and vorticity.shape[1] * 2 == CHUNKS
    )


def fast_on_device(*args):
    return fast_body(*args)


def fast_body(vorticity, divergence, trunc_cut, level_slot):
    planes = lax.axis_size("height")
    width = lax.axis_size("width")
    groups = lax.axis_size("row")
    columns = planes * width
    slots_local = vorticity.shape[1]
    waves = vorticity.shape[2]
    north_cells = vorticity.shape[3]
    east_cells = 2 * waves * columns
    rows_out = north_cells // (columns * groups)
    radix = rows_out // (SUBLANES // 2)
    height = lax.axis_index("height").astype(jnp.int32)
    column = height * width + lax.axis_index("width")
    place = jnp.stack([column * waves, height, column]).astype(jnp.int32)
    matrix, twiddle = north_tables(north_cells, radix, rows_out, columns * groups)
    cut = trunc_cut.reshape(1, waves)
    packed = radix * SUBLANES
    swaps = [[(z, z ^ j) for z in range(planes)] for j in range(planes)]
    order = list(range(planes - 1, 0, -1))

    def north(slot, wind, apart):
        return north_call(
            place, cut, vorticity, divergence, matrix, twiddle, slot, wind, radix, east_cells,
            planes, width * groups, apart,
        )

    def swap(parts):
        got = {0: parts[0]}
        for j in order:
            got[j] = lax.ppermute(parts[j], "height", swaps[j])
        return got

    def around(block):
        return lax.all_to_all(block, ("width", "row"), split_axis=0, concat_axis=0, tiled=True)

    chunks = [(slot, wind) for slot in range(slots_local) for wind in range(2)]
    table = east_table(waves, east_cells)
    outputs = [None, None]
    ready = []
    last = len(chunks) - 1
    for at, (slot, wind) in enumerate(chunks):
        if at == 0:
            swapped = swap(north(slot, wind, True))
            block = jnp.stack([swapped[j] for j in range(planes)], axis=1)
            block = around(block).reshape(width, groups, planes, packed, waves)
            ready.append((at, slot, wind, 0, groups, [(block, j) for j in range(planes)]))
        else:
            block = around(north(slot, wind, False)[0])
            block = block.reshape(width, groups, planes, packed, waves)
            pieces = LAST_PIECES if at == last else 1
            share = groups // pieces
            for piece in range(pieces):
                near = piece * share
                swapped = swap([block[:, near:near + share, j] for j in range(planes)])
                got = [(block, 0)] + [(swapped[j], None) for j in range(1, planes)]
                ready.append((at + piece, slot, wind, near, share, got))
    ready[0], ready[1] = ready[1], ready[0]
    for at, slot, wind, near, share, got in ready:
        outputs[wind] = east_call(
            place, level_slot, got, table, slot, slots_local, near, share, width, east_cells, waves, outputs[wind]
        )
    return (outputs[0][0], outputs[1][0], outputs[0][1], outputs[1][1])


def spectral_winds(vorticity, divergence, trunc_cut, first_wave, east_cells):
    local_count = vorticity.shape[2]
    north_cells = vorticity.shape[3]
    wave_index = first_wave + jnp.arange(local_count, dtype=jnp.int32)
    north_index = jnp.arange(north_cells, dtype=jnp.int32)
    north_wave = jnp.where(north_index < north_cells // 2, north_index, north_index - north_cells)
    wave_east = 2.0 * math.pi / east_cells * wave_index.astype(jnp.float32)
    wave_north = 2.0 * math.pi / north_cells * north_wave.astype(jnp.float32)
    east_col = wave_east[:, None]
    north_row = wave_north[None, :]
    square_wave = east_col * east_col + north_row * north_row
    retained = (jnp.abs(north_wave)[None, :] <= trunc_cut[:, None]) & (square_wave > 0)
    inverse_square = jnp.where(retained, 1.0 / jnp.where(square_wave > 0, square_wave, 1.0), 0.0)
    curl_real = vorticity[0]
    curl_imag = vorticity[1]
    source_real = divergence[0]
    source_imag = divergence[1]
    east_real = (-north_row * curl_imag + east_col * source_imag) * inverse_square
    east_imag = (north_row * curl_real - east_col * source_real) * inverse_square
    north_real = (east_col * curl_imag + north_row * source_imag) * inverse_square
    north_imag = (-east_col * curl_real - north_row * source_real) * inverse_square
    return jnp.stack([east_real, east_imag, north_real, north_imag], axis=1)


def north_transform(flattened, local_waves):
    slot_count = flattened.shape[0]
    north_cells = flattened.shape[2]
    block_size = math.gcd(north_cells, 256)
    block_count = north_cells // block_size
    north_index = jnp.arange(north_cells, dtype=jnp.int32)

    def north_one_block(block_index, result):
        row_index = block_index * block_size + jnp.arange(block_size, dtype=jnp.int32)
        phase_steps = row_index[:, None] * north_index[None, :] % north_cells
        angles = 2.0 * math.pi / north_cells * phase_steps.astype(jnp.float32)
        cosine_table = jnp.cos(angles)
        sine_table = jnp.sin(angles)
        with_cosine = jnp.einsum("yn,lkn->lyk", cosine_table, flattened, precision=HIGHEST)
        with_sine = jnp.einsum("yn,lkn->lyk", sine_table, flattened, precision=HIGHEST)
        with_cosine = with_cosine.reshape(slot_count, block_size, 2, 2, local_waves)
        with_sine = with_sine.reshape(slot_count, block_size, 2, 2, local_waves)
        real_part = with_cosine[:, :, :, 0] - with_sine[:, :, :, 1]
        imag_part = with_sine[:, :, :, 0] + with_cosine[:, :, :, 1]
        joined = jnp.concatenate([real_part, imag_part], axis=3)
        return lax.dynamic_update_slice_in_dim(result, joined, block_index * block_size, 1)

    initial = jnp.zeros((slot_count, north_cells, 2, 2 * local_waves), jnp.float32)
    return lax.fori_loop(0, block_count, north_one_block, initial)


def east_transform(stacked, local_waves, east_cells):
    columns = stacked.shape[0]
    slot_count = stacked.shape[1]
    row_count = stacked.shape[2]
    field_count = stacked.shape[3]
    block_size = math.gcd(east_cells, 256)
    block_count = east_cells // block_size
    wave_number = (
        jnp.arange(columns, dtype=jnp.int32)[:, None] * local_waves
        + jnp.arange(local_waves, dtype=jnp.int32)[None, :]
    )
    weights = jnp.where(wave_number == 0, 1.0, 2.0)[:, :, None]
    wave_east = 2.0 * math.pi / east_cells * wave_number.astype(jnp.float32)[:, :, None]

    def east_one_block(block_index, result):
        east_index = block_index * block_size + jnp.arange(block_size, dtype=jnp.int32)
        phase_steps = wave_number[:, :, None] * east_index[None, None, :] % east_cells
        angles = 2.0 * math.pi / east_cells * phase_steps.astype(jnp.float32)
        cosine_table = jnp.cos(angles)
        sine_table = jnp.sin(angles)
        value_real = weights * cosine_table
        value_imag = -weights * sine_table
        slope_real = -weights * wave_east * sine_table
        slope_imag = -weights * wave_east * cosine_table
        value_table = jnp.stack([value_real, value_imag], axis=1)
        slope_table = jnp.stack([slope_real, slope_imag], axis=1)
        east_table = jnp.stack([value_table, slope_table], axis=3).reshape(
            columns, 2 * local_waves, 2, block_size
        )
        product = jnp.einsum("clyfk,ckab->falyb", stacked, east_table, precision=HIGHEST)
        return lax.dynamic_update_slice_in_dim(result, product, block_index * block_size, 4)

    initial = jnp.zeros((field_count, 2, slot_count, row_count, east_cells), jnp.float32)
    return lax.fori_loop(0, block_count, east_one_block, initial)


def place_levels(grid_all, level_slot):
    slot_count = grid_all.shape[2]
    selector = (level_slot[None, :] == jnp.arange(slot_count, dtype=jnp.int32)[:, None]).astype(
        jnp.float32
    )
    return jnp.einsum("ls,fasyx->falyx", selector, grid_all, precision=HIGHEST)


def plain_on_device(vorticity, divergence, trunc_cut, level_slot):
    columns = lax.axis_size("col")
    row_count = lax.axis_size("row")
    local_waves = vorticity.shape[2]
    north_cells = vorticity.shape[3]
    east_cells = 2 * local_waves * columns
    first_wave = lax.axis_index("col") * local_waves
    spectra = spectral_winds(vorticity, divergence, trunc_cut, first_wave, east_cells)
    slot_count = spectra.shape[0]
    flattened = spectra.reshape(slot_count, 4 * local_waves, north_cells)
    fourier = north_transform(flattened, local_waves)
    outgoing = fourier[None]
    received = lax.all_to_all(outgoing, ("col", "row"), split_axis=2, concat_axis=0, tiled=True)
    shaped = received.reshape(
        columns,
        row_count * received.shape[1],
        received.shape[2],
        received.shape[3],
        received.shape[4],
    )
    grid_all = east_transform(shaped, local_waves, east_cells)
    placed = place_levels(grid_all, level_slot)
    return (placed[0, 0], placed[1, 0], placed[0, 1], placed[1, 1])


def solution(mesh):
    columns = mesh.shape["col"]
    groups = mesh.shape["row"]
    width = 2 if columns % 2 == 0 else 1
    fine = Mesh(mesh.devices.reshape(columns // width, width, groups), ("height", "width", "row"))

    def whole(vorticity, divergence, trunc_cut, level_slot):
        waves = vorticity.shape[2] // columns
        local = jax.ShapeDtypeStruct((2, vorticity.shape[1] // groups, waves, vorticity.shape[3]), F32)
        fast = fast_shapes(fine, local)
        column = ("height", "width") if fast else "col"
        grid = P(None, ("height", "width", "row") if fast else ("col", "row"), None)
        spectral = P(None, "row", column, None)
        return jax.shard_map(
            fast_on_device if fast else plain_on_device,
            mesh=fine if fast else mesh,
            in_specs=(spectral, spectral, P(column), P()),
            out_specs=(grid, grid, grid, grid),
            check_vma=False,
        )(vorticity, divergence, trunc_cut, level_slot)

    return whole
```

```python
import functools
import math

import jax
import jax.numpy as jnp
import numpy as np
from jax import lax
from jax.experimental import pallas as pl
from jax.experimental.pallas import tpu as pltpu
from jax.sharding import Mesh, PartitionSpec as P


HIGHEST = lax.Precision.HIGHEST
LANES = 128
SUBLANES = 8
EAST_RADIX = 8
CHUNKS = 4
FIRST_PICKS = 8
TURNS = (1, 0, 2, 3, 4)
F32 = jnp.float32
BF16 = jnp.bfloat16
ANY = pl.ANY


def cmul_root(value, k, n):
    re, im = value
    k = k % n
    if k == 0:
        return re, im
    if 4 * k == n:
        return -im, re
    if 2 * k == n:
        return -re, -im
    half = math.sqrt(0.5)
    if 8 * k == n:
        return (re - im) * half, (re + im) * half
    if 8 * k == 3 * n:
        return (re + im) * -half, (re - im) * half
    c = math.cos(2.0 * math.pi * k / n)
    s = math.sin(2.0 * math.pi * k / n)
    return re * c - im * s, re * s + im * c


def small_dft(values):
    n = len(values)
    if n == 1:
        return values
    even = small_dft(values[0::2])
    odd = small_dft(values[1::2])
    low, high = [], []
    for k in range(n // 2):
        er, ei = even[k]
        tr, ti = cmul_root(odd[k], k, n)
        low.append((er + tr, ei + ti))
        high.append((er - tr, ei - ti))
    return low + high


def small_dft_real(values):
    (r0, _), (r1, i1), (r2, i2), (r3, i3), (r4, _), (r5, i5), (r6, i6), (r7, i7) = values
    half = math.sqrt(0.5)
    s0, d0 = r0 + r4, r0 - r4
    s2, d2 = r2 + r6, i2 - i6
    s1r, d1r = r1 + r5, r1 - r5
    s1i, d1i = i1 + i5, i1 - i5
    s3r, d3r = r3 + r7, r3 - r7
    s3i, d3i = i3 + i7, i3 - i7
    p, q = s0 + s2, s1r + s3r
    e, f = s0 - s2, s1i - s3i
    g1r, g1i = (d1r - d1i) * half, (d1r + d1i) * half
    g3r, g3i = (d3r + d3i) * -half, (d3r - d3i) * half
    t, u = d0 - d2, g1r + g3r
    v, w = d0 + d2, g1i - g3i
    return [p + q, t + u, e - f, v - w, p - q, t - u, e + f, v + w]


def split_f32(value):
    high = value.astype(BF16)
    low = (value - high.astype(F32)).astype(BF16)
    return high, low


def north_tables(north_cells, radix, rows_out, devices):
    fast = north_cells // radix
    per_owner = rows_out // radix
    n2 = np.arange(fast)
    y2 = np.arange(devices)[:, None] * per_owner + np.arange(per_owner)[None, :]
    angle = 2.0 * np.pi / fast * ((y2[:, :, None] * n2[None, None, :]) % fast)
    c, s = np.cos(angle), np.sin(angle)
    real_rows = np.concatenate([c, -s], axis=2)
    imag_rows = np.concatenate([s, c], axis=2)
    matrix = np.concatenate([real_rows, imag_rows], axis=1).reshape(2 * fast, 2 * fast)
    matrix = matrix.astype(np.float32)
    high = matrix.astype(BF16)
    low = (matrix - high.astype(np.float32)).astype(BF16)
    turn = 2.0 * np.pi / north_cells * (np.arange(radix)[:, None] * n2[None, :])
    twiddle = np.stack([np.cos(turn), np.sin(turn)]).astype(np.float32)
    return np.stack([high, low]), twiddle


def place():
    height = lax.axis_index("height")
    return height, height * lax.axis_size("width") + lax.axis_index("width")


def north_kernel(
    wind, radix, first_pick, east_cells, north_cells, steps,
    cut_ref, vort_ref, div_ref, matrix_ref, twiddle_ref, *rest,
):
    *out_refs, cut_rows, winds, g_high, g_low = rest
    step = pl.program_id(0)
    height, column = place()
    waves = cut_ref.shape[1]
    picks = g_high.shape[0] // waves
    fast = north_cells // radix
    block_rows = vort_ref.shape[2]
    east_unit = 2.0 * math.pi / east_cells
    north_unit = 2.0 * math.pi / north_cells

    @pl.when(step == 0)
    def _():
        cut_rows[...] = jnp.broadcast_to(cut_ref[...], (LANES, waves)).T

    lane = lax.broadcasted_iota(jnp.int32, (SUBLANES, LANES), 1)
    sub = lax.broadcasted_iota(jnp.int32, (SUBLANES, LANES), 0)

    def wind_rows(part, carry):
        local = pl.multiple_of(part * SUBLANES, SUBLANES)
        base = pl.multiple_of(step * block_rows + local, SUBLANES)
        cut = cut_rows[pl.ds(base, SUBLANES), :]
        wave = column * waves + base + sub
        kx = east_unit * wave.astype(F32)
        kx2 = kx * kx
        weight = jnp.where(wave == 0, 1.0, 2.0).astype(F32)
        for n1 in range(radix):
            cols = slice(n1 * fast, (n1 + 1) * fast)
            index = lane + n1 * fast
            signed = jnp.where(index < north_cells // 2, index, index - north_cells)
            ky = north_unit * signed.astype(F32)
            square = kx2 + ky * ky
            positive = square > 0
            keep = (jnp.abs(signed) <= cut) & positive
            inverse = jnp.where(keep, weight / jnp.where(positive, square, 1.0), 0.0)
            zr = vort_ref[0, 0, pl.ds(local, SUBLANES), cols]
            zi = vort_ref[1, 0, pl.ds(local, SUBLANES), cols]
            dr = div_ref[0, 0, pl.ds(local, SUBLANES), cols]
            di = div_ref[1, 0, pl.ds(local, SUBLANES), cols]
            if wind == 0:
                re, im = kx * di - ky * zi, ky * zr - kx * dr
            else:
                re, im = kx * zi + ky * di, -kx * zr - ky * dr
            winds[0, n1, pl.ds(base, SUBLANES), :] = re * inverse
            winds[1, n1, pl.ds(base, SUBLANES), :] = im * inverse
        return carry

    lax.fori_loop(0, block_rows // SUBLANES, wind_rows, 0)

    @pl.when(step == steps - 1)
    def _():
        stride = EAST_RADIX
        count = waves // stride

        def transform(t, carry):
            residue = t ^ column
            values = []
            for n1 in range(radix):
                values.append(
                    tuple(winds[ri, n1, pl.ds(residue, count, stride=stride), :] for ri in range(2))
                )
            result = small_dft(values)
            for pick in range(picks):
                y1 = first_pick + pick
                re, im = result[y1]
                if y1:
                    c = twiddle_ref[0, y1:y1 + 1, :]
                    s = twiddle_ref[1, y1:y1 + 1, :]
                    re, im = re * c - im * s, re * s + im * c
                row = pl.multiple_of(pick * waves + t * count, count)
                high, low = split_f32(re)
                g_high[pl.ds(row, count), 0:fast] = high
                g_low[pl.ds(row, count), 0:fast] = low
                high, low = split_f32(im)
                g_high[pl.ds(row, count), fast:2 * fast] = high
                g_low[pl.ds(row, count), fast:2 * fast] = low
            return carry

        lax.fori_loop(0, stride, transform, 0)

    @pl.when(step == steps - 1)
    def _():
        contract = (((1,), (1,)), ((), ()))
        dot = functools.partial(lax.dot_general, dimension_numbers=contract, preferred_element_type=F32)
        planes = len(out_refs) if len(out_refs) > 1 else out_refs[0].shape[1]
        owners = out_refs[0].shape[0]
        span = owners * SUBLANES

        def rows_of(kind):
            return jnp.concatenate(
                [matrix_ref[kind, pl.ds((height ^ j) * span, span), :] for j in range(planes)], axis=0
            )

        matrix_high, matrix_low = rows_of(0), rows_of(1)
        for pair in range(picks // 2):
            rows = slice(pair * 2 * waves, (pair + 1) * 2 * waves)
            high = g_high[rows, :]
            low = g_low[rows, :]
            product = dot(matrix_high, high) + dot(matrix_high, low) + dot(matrix_low, high)
            for part in range(2):
                y1 = 2 * pair + part
                for j in range(planes):
                    piece = product[j * span:(j + 1) * span, part * waves:(part + 1) * waves]
                    piece = piece.reshape(owners, SUBLANES, waves)
                    if len(out_refs) > 1:
                        out_refs[j][:, y1] = piece
                    else:
                        out_refs[0][:, j, y1] = piece


def north_call(
    cut, vort, div, matrix, twiddle, slot, wind, radix, first_pick, picks, east_cells, planes, owners, apart
):
    waves = vort.shape[2]
    north_cells = vort.shape[3]
    steps = 2
    block_rows = waves // steps
    fast = north_cells // radix
    data_spec = pl.BlockSpec((2, 1, block_rows, north_cells), lambda i: (0, slot, i, 0))
    kernel = functools.partial(north_kernel, wind, radix, first_pick, east_cells, north_cells, steps)
    flops = 6 * (2 * fast) ** 2 * picks * waves
    tile = (picks, SUBLANES, waves)
    shape = (owners,) + tile if apart else (owners, planes) + tile
    whole = pl.BlockSpec(shape, lambda i: (0,) * len(shape))
    out_specs = [whole] * (planes if apart else 1)
    return pl.pallas_call(
        kernel,
        grid=(steps,),
        in_specs=[
            pl.BlockSpec((1, waves), lambda i: (0, 0)),
            data_spec,
            data_spec,
            pl.BlockSpec(matrix.shape, lambda i: (0, 0, 0)),
            pl.BlockSpec(twiddle.shape, lambda i: (0, 0, 0)),
        ],
        out_specs=out_specs,
        out_shape=[jax.ShapeDtypeStruct(shape, F32)] * len(out_specs),
        scratch_shapes=[
            pltpu.VMEM((waves, LANES), jnp.int32),
            pltpu.VMEM((2, radix, waves, fast), F32),
            pltpu.VMEM((picks * waves, 2 * fast), BF16),
            pltpu.VMEM((picks * waves, 2 * fast), BF16),
        ],
        compiler_params=pltpu.CompilerParams(dimension_semantics=("arbitrary",)),
        cost_estimate=pl.CostEstimate(flops=flops, bytes_accessed=6 << 20, transcendentals=0),
    )(cut, vort, div, matrix, twiddle)


def east_table(local_waves, east_cells):
    radix = EAST_RADIX
    span = east_cells // radix
    count = LANES // radix
    lane = jnp.arange(LANES, dtype=jnp.int32)[None, :]
    residue = jnp.arange(radix, dtype=jnp.int32)[:, None]
    wave = ((lane // count) ^ residue) * local_waves + (lane % count) * radix + residue
    steps = wave[:, :, None] * jnp.arange(span, dtype=jnp.int32)[None, None, :] % east_cells
    angle = 2.0 * math.pi / east_cells * steps.astype(F32)

    def parts(x):
        high = lax.reduce_precision(x, 8, 7)
        return jnp.stack([high.astype(BF16), (x - high).astype(BF16)], axis=1)

    c, s = parts(jnp.cos(angle)), parts(jnp.sin(angle))
    rows = [jnp.concatenate([c, s], axis=3), jnp.concatenate([-s, c], axis=3)]
    return jnp.concatenate(rows, axis=2)


def east_kernel(slot, slots_local, sources, first_group, east_cells, local_waves, *refs):
    planes = len(sources)
    level_ref, table = refs[:2]
    got_hbm = refs[2:2 + planes]
    value_ref, slope_ref, got, parts, spectra, grid_out, got_sems, out_sems = refs[-8:]
    radix = EAST_RADIX
    _, width, groups, packed, lanes = got.shape
    columns = planes * width
    north_radix = packed // SUBLANES
    per_owner = SUBLANES // 2
    rows_out = north_radix * per_owner
    span = spectra.shape[3] // 2
    height, _ = place()

    loads = []
    for j, plane in enumerate(sources):
        source = got_hbm[j]
        if plane is not None:
            source = source.at[:, pl.ds(first_group, groups), plane]
        copy = pltpu.make_async_copy(source, got.at[height ^ j], got_sems.at[j])
        copy.start()
        loads.append(copy)

    def columns_of(a):
        return slice(0, span if a % (radix // 2) == 0 else 2 * span)

    for copy in loads:
        copy.wait()

    lane = lax.broadcasted_iota(jnp.int32, (north_radix, lanes), 1)
    count = lanes // radix
    group_of = lane // count
    east_unit = 2.0 * math.pi / east_cells
    kx = [
        east_unit * ((group_of ^ a) * local_waves + (lane % count) * radix + a).astype(F32) for a in range(radix)
    ]

    def shuffle(group, carry):
        for y2 in range(per_owner):
            for ri in range(2):
                slabs = [
                    got[c // width, c % width, group, pl.ds(ri * per_owner + y2, north_radix, stride=SUBLANES), :]
                    for c in range(columns)
                ]
                bit = 1
                while bit < columns:
                    mask = (group_of & bit) == 0
                    slabs = [jnp.where(mask, slabs[i], slabs[i ^ bit]) for i in range(columns)]
                    bit *= 2
                row = pl.multiple_of(group * rows_out + y2 * north_radix, north_radix)
                for a in range(radix):
                    sloped = slabs[a] * kx[a]
                    for kind, value, part in ((0, slabs[a], ri), (1, -sloped if ri else sloped, 1 - ri)):
                        high, low = split_f32(value)
                        parts[a, kind, pl.ds(row, north_radix), part * lanes:(part + 1) * lanes] = high
                        parts[a, 2 + kind, pl.ds(row, north_radix), part * lanes:(part + 1) * lanes] = low
        return carry

    lax.fori_loop(0, groups, shuffle, 0)

    dot = functools.partial(jnp.dot, preferred_element_type=F32)

    def multiply(kind, a):
        cols = columns_of(a)
        left, left_low = parts[a, kind], parts[a, 2 + kind]
        right, right_low = table[a, 0, :, cols], table[a, 1, :, cols]
        spectra[kind, a, :, cols] = dot(left, right) + dot(left_low, right) + dot(left, right_low)

    def combine(kind, row):
        for tile in range(span // LANES):
            first = tile * LANES
            values = []
            for a in range(radix):
                re = spectra[kind, a, row:row + SUBLANES, first:first + LANES]
                im = None
                if a % (radix // 2):
                    im = spectra[kind, a, row:row + SUBLANES, first + span:first + span + LANES]
                values.append((re, im))
            outs = small_dft_real(values)
            for x1 in range(radix):
                at = x1 * span + first
                grid_out[kind, row:row + SUBLANES, at:at + LANES] = outs[x1]

    def finish(kind, group):
        for row in range(group * rows_out, (group + 1) * rows_out, SUBLANES):
            combine(kind, row)
        level = level_ref[(first_group + group) * slots_local + slot]
        copy = pltpu.make_async_copy(
            grid_out.at[kind, pl.ds(group * rows_out, rows_out), :],
            (value_ref, slope_ref)[kind].at[level],
            out_sems.at[2 * group + kind],
        )
        copy.start()
        return copy

    def multiply_both(a):
        cols = columns_of(a)
        rows = parts.shape[2]
        both = dot(parts[a].reshape(4 * rows, 2 * lanes), table[a, 0, :, cols])
        rest = dot(parts[a, 0:2].reshape(2 * rows, 2 * lanes), table[a, 1, :, cols])
        for kind in range(2):
            at, low = kind * rows, (2 + kind) * rows
            spectra[kind, a, :, cols] = both[at:at + rows] + both[low:low + rows] + rest[at:at + rows]

    together = groups == 1
    for a in range(radix):
        multiply_both(a) if together else multiply(0, a)
    copies = []
    for group in range(groups):
        if not together:
            for a in range(group * radix // groups, (group + 1) * radix // groups):
                multiply(1, a)
        copies.append(finish(0, group))
    for group in range(groups):
        copies.append(finish(1, group))
    for copy in copies:
        copy.wait()


def east_call(
    levels, got, table, slot, slots_local, first_group, groups, width, east_cells, local_waves, previous
):
    planes = len(got)
    packed, lanes = got[0][0].shape[-2:]
    rows_out = packed // 2
    radix = EAST_RADIX
    level_count = levels.shape[0]
    out = jax.ShapeDtypeStruct((level_count, rows_out, east_cells), F32)
    in_specs = [pl.BlockSpec(memory_space=pltpu.SMEM), pl.BlockSpec(memory_space=pltpu.VMEM)]
    in_specs += [pl.BlockSpec(memory_space=ANY)] * planes
    operands = [levels, table] + [array for array, _ in got]
    aliases = {}
    if previous is not None:
        aliases = {len(operands): 0, len(operands) + 1: 1}
        in_specs += [pl.BlockSpec(memory_space=ANY)] * 2
        operands += list(previous)
    rows = groups * rows_out
    columns = table.shape[-1]
    sources = tuple(plane for _, plane in got)
    return pl.pallas_call(
        functools.partial(east_kernel, slot, slots_local, sources, first_group, east_cells, local_waves),
        in_specs=in_specs,
        out_specs=[pl.BlockSpec(memory_space=ANY)] * 2,
        out_shape=[out, out],
        scratch_shapes=[
            pltpu.VMEM((planes, width, groups, packed, lanes), F32),
            pltpu.VMEM((radix, 4, rows, 2 * lanes), BF16),
            pltpu.VMEM((2, radix, rows, columns), F32),
            pltpu.VMEM((2, rows, east_cells), F32),
            pltpu.SemaphoreType.DMA((planes,)),
            pltpu.SemaphoreType.DMA((2 * groups,)),
        ],
        input_output_aliases=aliases,
        compiler_params=pltpu.CompilerParams(vmem_limit_bytes=40 << 20),
        cost_estimate=pl.CostEstimate(
            flops=12 * radix * rows * 2 * lanes * columns, bytes_accessed=14 << 20, transcendentals=0
        ),
    )(*operands)


def fast_shapes(mesh, vorticity):
    columns = mesh.shape["height"] * mesh.shape["width"]
    groups = mesh.shape["row"]
    waves = vorticity.shape[2]
    north_cells = vorticity.shape[3]
    rows_out = north_cells // (columns * groups)
    radix = rows_out // (SUBLANES // 2)
    return (
        waves == LANES
        and columns == EAST_RADIX
        and radix >= 2
        and radix & (radix - 1) == 0
        and north_cells == radix * LANES
        and radix > FIRST_PICKS
        and groups % 2 == 0
        and vorticity.shape[1] * 2 == CHUNKS
    )


def fast_on_device(*args):
    return fast_body(*args)


def fast_body(vorticity, divergence, trunc_cut, level_slot):
    planes = lax.axis_size("height")
    width = lax.axis_size("width")
    groups = lax.axis_size("row")
    columns = planes * width
    slots_local = vorticity.shape[1]
    waves = vorticity.shape[2]
    north_cells = vorticity.shape[3]
    east_cells = 2 * waves * columns
    rows_out = north_cells // (columns * groups)
    radix = rows_out // (SUBLANES // 2)
    matrix, twiddle = north_tables(north_cells, radix, rows_out, columns * groups)
    cut = trunc_cut.reshape(1, waves)
    packed = radix * SUBLANES
    swaps = [[(z, z ^ j) for z in range(planes)] for j in range(planes)]
    order = list(range(planes - 1, 0, -1))

    def north(slot, wind, first_pick, picks, apart):
        return north_call(
            cut, vorticity, divergence, matrix, twiddle, slot, wind, radix, first_pick, picks, east_cells,
            planes, width * groups, apart,
        )

    def swap(parts):
        got = {0: parts[0]}
        for j in order:
            got[j] = lax.ppermute(parts[j], "height", swaps[j])
        return got

    def around(block):
        return lax.all_to_all(block, ("width", "row"), split_axis=0, concat_axis=0, tiled=True)

    chunks = [(slot, wind) for slot in range(slots_local) for wind in range(2)]
    table = east_table(waves, east_cells)
    outputs = [None, None]
    ready = []
    last = len(chunks) - 1
    for at, (slot, wind) in enumerate(chunks):
        if at == 0:
            head = swap(north(slot, wind, 0, FIRST_PICKS, True))
            tail = swap(north(slot, wind, FIRST_PICKS, radix - FIRST_PICKS, True))
            joined = [jnp.concatenate([head[j], tail[j]], axis=1) for j in range(planes)]
            block = around(jnp.stack(joined, axis=1)).reshape(width, groups, planes, packed, waves)
            ready.append((at, slot, wind, 0, groups, [(block, j) for j in range(planes)]))
        else:
            block = around(north(slot, wind, 0, radix, False)[0])
            block = block.reshape(width, groups, planes, packed, waves)
            near = 0
            for piece, share in enumerate((groups // 2,) * 2 if at == last else (groups,)):
                swapped = swap([block[:, near:near + share, j] for j in range(planes)])
                got = [(block, 0)] + [(swapped[j], None) for j in range(1, planes)]
                ready.append((at + piece, slot, wind, near, share, got))
                near += share
    for at, slot, wind, near, share, got in (ready[turn] for turn in TURNS):
        outputs[wind] = east_call(
            level_slot, got, table, slot, slots_local, near, share, width, east_cells, waves, outputs[wind]
        )
    return (outputs[0][0], outputs[1][0], outputs[0][1], outputs[1][1])


def spectral_winds(vorticity, divergence, trunc_cut, first_wave, east_cells):
    local_count = vorticity.shape[2]
    north_cells = vorticity.shape[3]
    wave_index = first_wave + jnp.arange(local_count, dtype=jnp.int32)
    north_index = jnp.arange(north_cells, dtype=jnp.int32)
    north_wave = jnp.where(north_index < north_cells // 2, north_index, north_index - north_cells)
    wave_east = 2.0 * math.pi / east_cells * wave_index.astype(jnp.float32)
    wave_north = 2.0 * math.pi / north_cells * north_wave.astype(jnp.float32)
    east_col = wave_east[:, None]
    north_row = wave_north[None, :]
    square_wave = east_col * east_col + north_row * north_row
    retained = (jnp.abs(north_wave)[None, :] <= trunc_cut[:, None]) & (square_wave > 0)
    inverse_square = jnp.where(retained, 1.0 / jnp.where(square_wave > 0, square_wave, 1.0), 0.0)
    curl_real = vorticity[0]
    curl_imag = vorticity[1]
    source_real = divergence[0]
    source_imag = divergence[1]
    east_real = (-north_row * curl_imag + east_col * source_imag) * inverse_square
    east_imag = (north_row * curl_real - east_col * source_real) * inverse_square
    north_real = (east_col * curl_imag + north_row * source_imag) * inverse_square
    north_imag = (-east_col * curl_real - north_row * source_real) * inverse_square
    return jnp.stack([east_real, east_imag, north_real, north_imag], axis=1)


def north_transform(flattened, local_waves):
    slot_count = flattened.shape[0]
    north_cells = flattened.shape[2]
    block_size = math.gcd(north_cells, 256)
    block_count = north_cells // block_size
    north_index = jnp.arange(north_cells, dtype=jnp.int32)

    def north_one_block(block_index, result):
        row_index = block_index * block_size + jnp.arange(block_size, dtype=jnp.int32)
        phase_steps = row_index[:, None] * north_index[None, :] % north_cells
        angles = 2.0 * math.pi / north_cells * phase_steps.astype(jnp.float32)
        cosine_table = jnp.cos(angles)
        sine_table = jnp.sin(angles)
        with_cosine = jnp.einsum("yn,lkn->lyk", cosine_table, flattened, precision=HIGHEST)
        with_sine = jnp.einsum("yn,lkn->lyk", sine_table, flattened, precision=HIGHEST)
        with_cosine = with_cosine.reshape(slot_count, block_size, 2, 2, local_waves)
        with_sine = with_sine.reshape(slot_count, block_size, 2, 2, local_waves)
        real_part = with_cosine[:, :, :, 0] - with_sine[:, :, :, 1]
        imag_part = with_sine[:, :, :, 0] + with_cosine[:, :, :, 1]
        joined = jnp.concatenate([real_part, imag_part], axis=3)
        return lax.dynamic_update_slice_in_dim(result, joined, block_index * block_size, 1)

    initial = jnp.zeros((slot_count, north_cells, 2, 2 * local_waves), jnp.float32)
    return lax.fori_loop(0, block_count, north_one_block, initial)


def east_transform(stacked, local_waves, east_cells):
    columns = stacked.shape[0]
    slot_count = stacked.shape[1]
    row_count = stacked.shape[2]
    field_count = stacked.shape[3]
    block_size = math.gcd(east_cells, 256)
    block_count = east_cells // block_size
    wave_number = (
        jnp.arange(columns, dtype=jnp.int32)[:, None] * local_waves
        + jnp.arange(local_waves, dtype=jnp.int32)[None, :]
    )
    weights = jnp.where(wave_number == 0, 1.0, 2.0)[:, :, None]
    wave_east = 2.0 * math.pi / east_cells * wave_number.astype(jnp.float32)[:, :, None]

    def east_one_block(block_index, result):
        east_index = block_index * block_size + jnp.arange(block_size, dtype=jnp.int32)
        phase_steps = wave_number[:, :, None] * east_index[None, None, :] % east_cells
        angles = 2.0 * math.pi / east_cells * phase_steps.astype(jnp.float32)
        cosine_table = jnp.cos(angles)
        sine_table = jnp.sin(angles)
        value_real = weights * cosine_table
        value_imag = -weights * sine_table
        slope_real = -weights * wave_east * sine_table
        slope_imag = -weights * wave_east * cosine_table
        value_table = jnp.stack([value_real, value_imag], axis=1)
        slope_table = jnp.stack([slope_real, slope_imag], axis=1)
        east_table = jnp.stack([value_table, slope_table], axis=3).reshape(
            columns, 2 * local_waves, 2, block_size
        )
        product = jnp.einsum("clyfk,ckab->falyb", stacked, east_table, precision=HIGHEST)
        return lax.dynamic_update_slice_in_dim(result, product, block_index * block_size, 4)

    initial = jnp.zeros((field_count, 2, slot_count, row_count, east_cells), jnp.float32)
    return lax.fori_loop(0, block_count, east_one_block, initial)


def place_levels(grid_all, level_slot):
    slot_count = grid_all.shape[2]
    selector = (level_slot[None, :] == jnp.arange(slot_count, dtype=jnp.int32)[:, None]).astype(
        jnp.float32
    )
    return jnp.einsum("ls,fasyx->falyx", selector, grid_all, precision=HIGHEST)


def plain_on_device(vorticity, divergence, trunc_cut, level_slot):
    columns = lax.axis_size("col")
    row_count = lax.axis_size("row")
    local_waves = vorticity.shape[2]
    north_cells = vorticity.shape[3]
    east_cells = 2 * local_waves * columns
    first_wave = lax.axis_index("col") * local_waves
    spectra = spectral_winds(vorticity, divergence, trunc_cut, first_wave, east_cells)
    slot_count = spectra.shape[0]
    flattened = spectra.reshape(slot_count, 4 * local_waves, north_cells)
    fourier = north_transform(flattened, local_waves)
    outgoing = fourier[None]
    received = lax.all_to_all(outgoing, ("col", "row"), split_axis=2, concat_axis=0, tiled=True)
    shaped = received.reshape(
        columns,
        row_count * received.shape[1],
        received.shape[2],
        received.shape[3],
        received.shape[4],
    )
    grid_all = east_transform(shaped, local_waves, east_cells)
    placed = place_levels(grid_all, level_slot)
    return (placed[0, 0], placed[1, 0], placed[0, 1], placed[1, 1])


def solution(mesh):
    columns = mesh.shape["col"]
    groups = mesh.shape["row"]
    width = 2 if columns % 2 == 0 else 1
    fine = Mesh(mesh.devices.reshape(columns // width, width, groups), ("height", "width", "row"))

    def whole(vorticity, divergence, trunc_cut, level_slot):
        waves = vorticity.shape[2] // columns
        local = jax.ShapeDtypeStruct((2, vorticity.shape[1] // groups, waves, vorticity.shape[3]), F32)
        fast = fast_shapes(fine, local)
        column = ("height", "width") if fast else "col"
        grid = P(None, ("height", "width", "row") if fast else ("col", "row"), None)
        spectral = P(None, "row", column, None)
        return jax.shard_map(
            fast_on_device if fast else plain_on_device,
            mesh=fine if fast else mesh,
            in_specs=(spectral, spectral, P(column), P()),
            out_specs=(grid, grid, grid, grid),
            check_vma=False,
        )(vorticity, divergence, trunc_cut, level_slot)

    return whole
```

```python
import functools
import math

import jax
import jax.numpy as jnp
import numpy as np
from jax import lax
from jax.experimental import pallas as pl
from jax.experimental.pallas import tpu as pltpu
from jax.sharding import Mesh, PartitionSpec as P


HIGHEST = lax.Precision.HIGHEST
LANES = 128
SUBLANES = 8
EAST_RADIX = 8
CHUNKS = 4
FIRST_PICKS = 8
TURNS = (1, 0, 2, 3, 4)
F32 = jnp.float32
BF16 = jnp.bfloat16
ANY = pl.ANY


def cmul_root(value, k, n):
    re, im = value
    k = k % n
    if k == 0:
        return re, im
    if 4 * k == n:
        return -im, re
    if 2 * k == n:
        return -re, -im
    half = math.sqrt(0.5)
    if 8 * k == n:
        return (re - im) * half, (re + im) * half
    if 8 * k == 3 * n:
        return (re + im) * -half, (re - im) * half
    c = math.cos(2.0 * math.pi * k / n)
    s = math.sin(2.0 * math.pi * k / n)
    return re * c - im * s, re * s + im * c


def small_dft(values):
    n = len(values)
    if n == 1:
        return values
    even = small_dft(values[0::2])
    odd = small_dft(values[1::2])
    low, high = [], []
    for k in range(n // 2):
        er, ei = even[k]
        tr, ti = cmul_root(odd[k], k, n)
        low.append((er + tr, ei + ti))
        high.append((er - tr, ei - ti))
    return low + high


def small_dft_real(values):
    (r0, _), (r1, i1), (r2, i2), (r3, i3), (r4, _), (r5, i5), (r6, i6), (r7, i7) = values
    half = math.sqrt(0.5)
    s0, d0 = r0 + r4, r0 - r4
    s2, d2 = r2 + r6, i2 - i6
    s1r, d1r = r1 + r5, r1 - r5
    s1i, d1i = i1 + i5, i1 - i5
    s3r, d3r = r3 + r7, r3 - r7
    s3i, d3i = i3 + i7, i3 - i7
    p, q = s0 + s2, s1r + s3r
    e, f = s0 - s2, s1i - s3i
    g1r, g1i = (d1r - d1i) * half, (d1r + d1i) * half
    g3r, g3i = (d3r + d3i) * -half, (d3r - d3i) * half
    t, u = d0 - d2, g1r + g3r
    v, w = d0 + d2, g1i - g3i
    return [p + q, t + u, e - f, v - w, p - q, t - u, e + f, v + w]


def split_f32(value):
    high = value.astype(BF16)
    low = (value - high.astype(F32)).astype(BF16)
    return high, low


def north_tables(north_cells, radix, rows_out, devices):
    fast = north_cells // radix
    per_owner = rows_out // radix
    n2 = np.arange(fast)
    y2 = np.arange(devices)[:, None] * per_owner + np.arange(per_owner)[None, :]
    angle = 2.0 * np.pi / fast * ((y2[:, :, None] * n2[None, None, :]) % fast)
    c, s = np.cos(angle), np.sin(angle)
    real_rows = np.concatenate([c, -s], axis=2)
    imag_rows = np.concatenate([s, c], axis=2)
    matrix = np.concatenate([real_rows, imag_rows], axis=1).reshape(2 * fast, 2 * fast)
    matrix = matrix.astype(np.float32)
    high = matrix.astype(BF16)
    low = (matrix - high.astype(np.float32)).astype(BF16)
    turn = 2.0 * np.pi / north_cells * (np.arange(radix)[:, None] * n2[None, :])
    twiddle = np.stack([np.cos(turn), np.sin(turn)]).astype(np.float32)
    return np.stack([high, low]), twiddle


def place():
    height = lax.axis_index("height")
    return height, height * lax.axis_size("width") + lax.axis_index("width")


def north_kernel(
    wind, radix, first_pick, east_cells, north_cells, steps,
    cut_ref, vort_ref, div_ref, matrix_ref, twiddle_ref, *rest,
):
    *out_refs, cut_rows, winds, g_high, g_low = rest
    step = pl.program_id(0)
    height, column = place()
    waves = cut_ref.shape[1]
    picks = g_high.shape[0] // waves
    fast = north_cells // radix
    block_rows = vort_ref.shape[2]
    east_unit = 2.0 * math.pi / east_cells
    north_unit = 2.0 * math.pi / north_cells

    @pl.when(step == 0)
    def _():
        cut_rows[...] = jnp.broadcast_to(cut_ref[...], (LANES, waves)).T

    lane = lax.broadcasted_iota(jnp.int32, (SUBLANES, LANES), 1)
    sub = lax.broadcasted_iota(jnp.int32, (SUBLANES, LANES), 0)

    def wind_rows(part, carry):
        local = pl.multiple_of(part * SUBLANES, SUBLANES)
        base = pl.multiple_of(step * block_rows + local, SUBLANES)
        cut = cut_rows[pl.ds(base, SUBLANES), :]
        wave = column * waves + base + sub
        kx = east_unit * wave.astype(F32)
        kx2 = kx * kx
        weight = jnp.where(wave == 0, 1.0, 2.0).astype(F32)
        for n1 in range(radix):
            cols = slice(n1 * fast, (n1 + 1) * fast)
            index = lane + n1 * fast
            signed = jnp.where(index < north_cells // 2, index, index - north_cells)
            ky = north_unit * signed.astype(F32)
            square = kx2 + ky * ky
            positive = square > 0
            keep = (jnp.abs(signed) <= cut) & positive
            inverse = jnp.where(keep, weight / jnp.where(positive, square, 1.0), 0.0)
            zr = vort_ref[0, 0, pl.ds(local, SUBLANES), cols]
            zi = vort_ref[1, 0, pl.ds(local, SUBLANES), cols]
            dr = div_ref[0, 0, pl.ds(local, SUBLANES), cols]
            di = div_ref[1, 0, pl.ds(local, SUBLANES), cols]
            if wind == 0:
                re, im = kx * di - ky * zi, ky * zr - kx * dr
            else:
                re, im = kx * zi + ky * di, -kx * zr - ky * dr
            winds[0, n1, pl.ds(base, SUBLANES), :] = re * inverse
            winds[1, n1, pl.ds(base, SUBLANES), :] = im * inverse
        return carry

    lax.fori_loop(0, block_rows // SUBLANES, wind_rows, 0)

    @pl.when(step == steps - 1)
    def _():
        stride = EAST_RADIX
        count = waves // stride

        def transform(t, carry):
            residue = t ^ column
            values = []
            for n1 in range(radix):
                values.append(
                    tuple(winds[ri, n1, pl.ds(residue, count, stride=stride), :] for ri in range(2))
                )
            result = small_dft(values)
            for pick in range(picks):
                y1 = first_pick + pick
                re, im = result[y1]
                if y1:
                    c = twiddle_ref[0, y1:y1 + 1, :]
                    s = twiddle_ref[1, y1:y1 + 1, :]
                    re, im = re * c - im * s, re * s + im * c
                row = pl.multiple_of(pick * waves + t * count, count)
                high, low = split_f32(re)
                g_high[pl.ds(row, count), 0:fast] = high
                g_low[pl.ds(row, count), 0:fast] = low
                high, low = split_f32(im)
                g_high[pl.ds(row, count), fast:2 * fast] = high
                g_low[pl.ds(row, count), fast:2 * fast] = low
            return carry

        lax.fori_loop(0, stride, transform, 0)

    @pl.when(step == steps - 1)
    def _():
        contract = (((1,), (1,)), ((), ()))
        dot = functools.partial(lax.dot_general, dimension_numbers=contract, preferred_element_type=F32)
        planes = len(out_refs) if len(out_refs) > 1 else out_refs[0].shape[1]
        owners = out_refs[0].shape[0]
        span = owners * SUBLANES

        def rows_of(kind):
            return jnp.concatenate(
                [matrix_ref[kind, pl.ds((height ^ j) * span, span), :] for j in range(planes)], axis=0
            )

        matrix_high, matrix_low = rows_of(0), rows_of(1)
        for pair in range(picks // 2):
            rows = slice(pair * 2 * waves, (pair + 1) * 2 * waves)
            high = g_high[rows, :]
            low = g_low[rows, :]
            product = dot(matrix_high, high) + dot(matrix_high, low) + dot(matrix_low, high)
            for part in range(2):
                y1 = 2 * pair + part
                for j in range(planes):
                    piece = product[j * span:(j + 1) * span, part * waves:(part + 1) * waves]
                    piece = piece.reshape(owners, SUBLANES, waves)
                    if len(out_refs) > 1:
                        out_refs[j][:, y1] = piece
                    else:
                        out_refs[0][:, j, y1] = piece


def north_call(
    cut, vort, div, matrix, twiddle, slot, wind, radix, first_pick, picks, east_cells, planes, owners, apart
):
    waves = vort.shape[2]
    north_cells = vort.shape[3]
    steps = 2
    block_rows = waves // steps
    fast = north_cells // radix
    data_spec = pl.BlockSpec((2, 1, block_rows, north_cells), lambda i: (0, slot, i, 0))
    kernel = functools.partial(north_kernel, wind, radix, first_pick, east_cells, north_cells, steps)
    flops = 6 * (2 * fast) ** 2 * picks * waves
    tile = (picks, SUBLANES, waves)
    shape = (owners,) + tile if apart else (owners, planes) + tile
    whole = pl.BlockSpec(shape, lambda i: (0,) * len(shape))
    out_specs = [whole] * (planes if apart else 1)
    return pl.pallas_call(
        kernel,
        grid=(steps,),
        in_specs=[
            pl.BlockSpec((1, waves), lambda i: (0, 0)),
            data_spec,
            data_spec,
            pl.BlockSpec(matrix.shape, lambda i: (0, 0, 0)),
            pl.BlockSpec(twiddle.shape, lambda i: (0, 0, 0)),
        ],
        out_specs=out_specs,
        out_shape=[jax.ShapeDtypeStruct(shape, F32)] * len(out_specs),
        scratch_shapes=[
            pltpu.VMEM((waves, LANES), jnp.int32),
            pltpu.VMEM((2, radix, waves, fast), F32),
            pltpu.VMEM((picks * waves, 2 * fast), BF16),
            pltpu.VMEM((picks * waves, 2 * fast), BF16),
        ],
        compiler_params=pltpu.CompilerParams(dimension_semantics=("arbitrary",)),
        cost_estimate=pl.CostEstimate(flops=flops, bytes_accessed=6 << 20, transcendentals=0),
    )(cut, vort, div, matrix, twiddle)


def east_table(local_waves, east_cells):
    radix = EAST_RADIX
    span = east_cells // radix
    count = LANES // radix
    lane = jnp.arange(LANES, dtype=jnp.int32)[None, :]
    residue = jnp.arange(radix, dtype=jnp.int32)[:, None]
    wave = ((lane // count) ^ residue) * local_waves + (lane % count) * radix + residue
    steps = wave[:, :, None] * jnp.arange(span, dtype=jnp.int32)[None, None, :] % east_cells
    angle = 2.0 * math.pi / east_cells * steps.astype(F32)

    def parts(x):
        high = lax.reduce_precision(x, 8, 7)
        return jnp.stack([high.astype(BF16), (x - high).astype(BF16)], axis=1)

    c, s = parts(jnp.cos(angle)), parts(jnp.sin(angle))
    rows = [jnp.concatenate([c, s], axis=3), jnp.concatenate([-s, c], axis=3)]
    return jnp.concatenate(rows, axis=2)


def east_kernel(slot, slots_local, sources, first_group, east_cells, local_waves, *refs):
    planes = len(sources)
    level_ref, table = refs[:2]
    got_hbm = refs[2:2 + planes]
    value_ref, slope_ref, got, parts, spectra, grid_out, got_sems, out_sems = refs[-8:]
    radix = EAST_RADIX
    _, width, groups, packed, lanes = got.shape
    columns = planes * width
    north_radix = packed // SUBLANES
    per_owner = SUBLANES // 2
    rows_out = north_radix * per_owner
    span = spectra.shape[3] // 2
    height, _ = place()

    loads = []
    for j, plane in enumerate(sources):
        source = got_hbm[j]
        if plane is not None:
            source = source.at[:, pl.ds(first_group, groups), plane]
        copy = pltpu.make_async_copy(source, got.at[height ^ j], got_sems.at[j])
        copy.start()
        loads.append(copy)

    def columns_of(a):
        return slice(0, span if a % (radix // 2) == 0 else 2 * span)

    for copy in loads:
        copy.wait()

    lane = lax.broadcasted_iota(jnp.int32, (north_radix, lanes), 1)
    count = lanes // radix
    group_of = lane // count
    east_unit = 2.0 * math.pi / east_cells
    kx = [
        east_unit * ((group_of ^ a) * local_waves + (lane % count) * radix + a).astype(F32) for a in range(radix)
    ]

    def shuffle(group, carry):
        for y2 in range(per_owner):
            for ri in range(2):
                slabs = [
                    got[c // width, c % width, group, pl.ds(ri * per_owner + y2, north_radix, stride=SUBLANES), :]
                    for c in range(columns)
                ]
                bit = 1
                while bit < columns:
                    mask = (group_of & bit) == 0
                    slabs = [jnp.where(mask, slabs[i], slabs[i ^ bit]) for i in range(columns)]
                    bit *= 2
                row = pl.multiple_of(group * rows_out + y2 * north_radix, north_radix)
                for a in range(radix):
                    sloped = slabs[a] * kx[a]
                    for kind, value, part in ((0, slabs[a], ri), (1, -sloped if ri else sloped, 1 - ri)):
                        high, low = split_f32(value)
                        parts[a, kind, pl.ds(row, north_radix), part * lanes:(part + 1) * lanes] = high
                        parts[a, 2 + kind, pl.ds(row, north_radix), part * lanes:(part + 1) * lanes] = low
        return carry

    lax.fori_loop(0, groups, shuffle, 0)

    dot = functools.partial(jnp.dot, preferred_element_type=F32)

    def multiply(kind, a):
        cols = columns_of(a)
        left, left_low = parts[a, kind], parts[a, 2 + kind]
        right, right_low = table[a, 0, :, cols], table[a, 1, :, cols]
        spectra[kind, a, :, cols] = dot(left, right) + dot(left_low, right) + dot(left, right_low)

    def combine(kind, row):
        for tile in range(span // LANES):
            first = tile * LANES
            values = []
            for a in range(radix):
                re = spectra[kind, a, row:row + SUBLANES, first:first + LANES]
                im = None
                if a % (radix // 2):
                    im = spectra[kind, a, row:row + SUBLANES, first + span:first + span + LANES]
                values.append((re, im))
            outs = small_dft_real(values)
            for x1 in range(radix):
                at = x1 * span + first
                grid_out[kind, row:row + SUBLANES, at:at + LANES] = outs[x1]

    def finish(kind, group):
        for row in range(group * rows_out, (group + 1) * rows_out, SUBLANES):
            combine(kind, row)
        level = level_ref[(first_group + group) * slots_local + slot]
        copy = pltpu.make_async_copy(
            grid_out.at[kind, pl.ds(group * rows_out, rows_out), :],
            (value_ref, slope_ref)[kind].at[level],
            out_sems.at[2 * group + kind],
        )
        copy.start()
        return copy

    def multiply_both(a):
        cols = columns_of(a)
        rows = parts.shape[2]
        both = dot(parts[a].reshape(4 * rows, 2 * lanes), table[a, 0, :, cols])
        rest = dot(parts[a, 0:2].reshape(2 * rows, 2 * lanes), table[a, 1, :, cols])
        for kind in range(2):
            at, low = kind * rows, (2 + kind) * rows
            spectra[kind, a, :, cols] = both[at:at + rows] + both[low:low + rows] + rest[at:at + rows]

    together = groups == 1
    for a in range(radix):
        multiply_both(a) if together else multiply(0, a)
    copies = []
    for group in range(groups):
        if not together:
            for a in range(group * radix // groups, (group + 1) * radix // groups):
                multiply(1, a)
        copies.append(finish(0, group))
    for group in range(groups):
        copies.append(finish(1, group))
    for copy in copies:
        copy.wait()


def east_call(
    levels, got, table, slot, slots_local, first_group, groups, width, east_cells, local_waves, previous
):
    planes = len(got)
    packed, lanes = got[0][0].shape[-2:]
    rows_out = packed // 2
    radix = EAST_RADIX
    level_count = levels.shape[0]
    out = jax.ShapeDtypeStruct((level_count, rows_out, east_cells), F32)
    in_specs = [pl.BlockSpec(memory_space=pltpu.SMEM), pl.BlockSpec(memory_space=pltpu.VMEM)]
    in_specs += [pl.BlockSpec(memory_space=ANY)] * planes
    operands = [levels, table] + [array for array, _ in got]
    aliases = {}
    if previous is not None:
        aliases = {len(operands): 0, len(operands) + 1: 1}
        in_specs += [pl.BlockSpec(memory_space=ANY)] * 2
        operands += list(previous)
    rows = groups * rows_out
    columns = table.shape[-1]
    sources = tuple(plane for _, plane in got)
    return pl.pallas_call(
        functools.partial(east_kernel, slot, slots_local, sources, first_group, east_cells, local_waves),
        in_specs=in_specs,
        out_specs=[pl.BlockSpec(memory_space=ANY)] * 2,
        out_shape=[out, out],
        scratch_shapes=[
            pltpu.VMEM((planes, width, groups, packed, lanes), F32),
            pltpu.VMEM((radix, 4, rows, 2 * lanes), BF16),
            pltpu.VMEM((2, radix, rows, columns), F32),
            pltpu.VMEM((2, rows, east_cells), F32),
            pltpu.SemaphoreType.DMA((planes,)),
            pltpu.SemaphoreType.DMA((2 * groups,)),
        ],
        input_output_aliases=aliases,
        compiler_params=pltpu.CompilerParams(vmem_limit_bytes=40 << 20),
        cost_estimate=pl.CostEstimate(
            flops=12 * radix * rows * 2 * lanes * columns, bytes_accessed=14 << 20, transcendentals=0
        ),
    )(*operands)


def fast_shapes(mesh, vorticity):
    columns = mesh.shape["height"] * mesh.shape["width"]
    groups = mesh.shape["row"]
    waves = vorticity.shape[2]
    north_cells = vorticity.shape[3]
    rows_out = north_cells // (columns * groups)
    radix = rows_out // (SUBLANES // 2)
    return (
        waves == LANES
        and columns == EAST_RADIX
        and radix >= 2
        and radix & (radix - 1) == 0
        and north_cells == radix * LANES
        and radix > FIRST_PICKS
        and groups % 2 == 0
        and vorticity.shape[1] * 2 == CHUNKS
    )


def swap_order(planes):
    half = planes // 2
    return [half] + [j for j in range(planes - 1, 0, -1) if j != half]


def fast_on_device(*args):
    return fast_body(*args)


def fast_body(vorticity, divergence, trunc_cut, level_slot):
    planes = lax.axis_size("height")
    width = lax.axis_size("width")
    groups = lax.axis_size("row")
    columns = planes * width
    slots_local = vorticity.shape[1]
    waves = vorticity.shape[2]
    north_cells = vorticity.shape[3]
    east_cells = 2 * waves * columns
    rows_out = north_cells // (columns * groups)
    radix = rows_out // (SUBLANES // 2)
    matrix, twiddle = north_tables(north_cells, radix, rows_out, columns * groups)
    cut = trunc_cut.reshape(1, waves)
    packed = radix * SUBLANES
    swaps = [[(z, z ^ j) for z in range(planes)] for j in range(planes)]
    order = swap_order(planes)

    def north(slot, wind, first_pick, picks, apart):
        return north_call(
            cut, vorticity, divergence, matrix, twiddle, slot, wind, radix, first_pick, picks, east_cells,
            planes, width * groups, apart,
        )

    def swap(parts):
        got = {0: parts[0]}
        for j in order:
            got[j] = lax.ppermute(parts[j], "height", swaps[j])
        return got

    def around(block):
        return lax.all_to_all(block, ("width", "row"), split_axis=0, concat_axis=0, tiled=True)

    chunks = [(slot, wind) for slot in range(slots_local) for wind in range(2)]
    table = east_table(waves, east_cells)
    outputs = [None, None]
    ready = []
    last = len(chunks) - 1
    for at, (slot, wind) in enumerate(chunks):
        if at == 0:
            head = swap(north(slot, wind, 0, FIRST_PICKS, True))
            tail = swap(north(slot, wind, FIRST_PICKS, radix - FIRST_PICKS, True))
            joined = [jnp.concatenate([head[j], tail[j]], axis=1) for j in range(planes)]
            block = around(jnp.stack(joined, axis=1)).reshape(width, groups, planes, packed, waves)
            ready.append((at, slot, wind, 0, groups, [(block, j) for j in range(planes)]))
        else:
            block = around(north(slot, wind, 0, radix, False)[0])
            block = block.reshape(width, groups, planes, packed, waves)
            near = 0
            for piece, share in enumerate((groups // 2,) * 2 if at == last else (groups,)):
                swapped = swap([block[:, near:near + share, j] for j in range(planes)])
                got = [(block, 0)] + [(swapped[j], None) for j in range(1, planes)]
                ready.append((at + piece, slot, wind, near, share, got))
                near += share
    for at, slot, wind, near, share, got in (ready[turn] for turn in TURNS):
        outputs[wind] = east_call(
            level_slot, got, table, slot, slots_local, near, share, width, east_cells, waves, outputs[wind]
        )
    return (outputs[0][0], outputs[1][0], outputs[0][1], outputs[1][1])


def spectral_winds(vorticity, divergence, trunc_cut, first_wave, east_cells):
    local_count = vorticity.shape[2]
    north_cells = vorticity.shape[3]
    wave_index = first_wave + jnp.arange(local_count, dtype=jnp.int32)
    north_index = jnp.arange(north_cells, dtype=jnp.int32)
    north_wave = jnp.where(north_index < north_cells // 2, north_index, north_index - north_cells)
    wave_east = 2.0 * math.pi / east_cells * wave_index.astype(jnp.float32)
    wave_north = 2.0 * math.pi / north_cells * north_wave.astype(jnp.float32)
    east_col = wave_east[:, None]
    north_row = wave_north[None, :]
    square_wave = east_col * east_col + north_row * north_row
    retained = (jnp.abs(north_wave)[None, :] <= trunc_cut[:, None]) & (square_wave > 0)
    inverse_square = jnp.where(retained, 1.0 / jnp.where(square_wave > 0, square_wave, 1.0), 0.0)
    curl_real = vorticity[0]
    curl_imag = vorticity[1]
    source_real = divergence[0]
    source_imag = divergence[1]
    east_real = (-north_row * curl_imag + east_col * source_imag) * inverse_square
    east_imag = (north_row * curl_real - east_col * source_real) * inverse_square
    north_real = (east_col * curl_imag + north_row * source_imag) * inverse_square
    north_imag = (-east_col * curl_real - north_row * source_real) * inverse_square
    return jnp.stack([east_real, east_imag, north_real, north_imag], axis=1)


def north_transform(flattened, local_waves):
    slot_count = flattened.shape[0]
    north_cells = flattened.shape[2]
    block_size = math.gcd(north_cells, 256)
    block_count = north_cells // block_size
    north_index = jnp.arange(north_cells, dtype=jnp.int32)

    def north_one_block(block_index, result):
        row_index = block_index * block_size + jnp.arange(block_size, dtype=jnp.int32)
        phase_steps = row_index[:, None] * north_index[None, :] % north_cells
        angles = 2.0 * math.pi / north_cells * phase_steps.astype(jnp.float32)
        cosine_table = jnp.cos(angles)
        sine_table = jnp.sin(angles)
        with_cosine = jnp.einsum("yn,lkn->lyk", cosine_table, flattened, precision=HIGHEST)
        with_sine = jnp.einsum("yn,lkn->lyk", sine_table, flattened, precision=HIGHEST)
        with_cosine = with_cosine.reshape(slot_count, block_size, 2, 2, local_waves)
        with_sine = with_sine.reshape(slot_count, block_size, 2, 2, local_waves)
        real_part = with_cosine[:, :, :, 0] - with_sine[:, :, :, 1]
        imag_part = with_sine[:, :, :, 0] + with_cosine[:, :, :, 1]
        joined = jnp.concatenate([real_part, imag_part], axis=3)
        return lax.dynamic_update_slice_in_dim(result, joined, block_index * block_size, 1)

    initial = jnp.zeros((slot_count, north_cells, 2, 2 * local_waves), jnp.float32)
    return lax.fori_loop(0, block_count, north_one_block, initial)


def east_transform(stacked, local_waves, east_cells):
    columns = stacked.shape[0]
    slot_count = stacked.shape[1]
    row_count = stacked.shape[2]
    field_count = stacked.shape[3]
    block_size = math.gcd(east_cells, 256)
    block_count = east_cells // block_size
    wave_number = (
        jnp.arange(columns, dtype=jnp.int32)[:, None] * local_waves
        + jnp.arange(local_waves, dtype=jnp.int32)[None, :]
    )
    weights = jnp.where(wave_number == 0, 1.0, 2.0)[:, :, None]
    wave_east = 2.0 * math.pi / east_cells * wave_number.astype(jnp.float32)[:, :, None]

    def east_one_block(block_index, result):
        east_index = block_index * block_size + jnp.arange(block_size, dtype=jnp.int32)
        phase_steps = wave_number[:, :, None] * east_index[None, None, :] % east_cells
        angles = 2.0 * math.pi / east_cells * phase_steps.astype(jnp.float32)
        cosine_table = jnp.cos(angles)
        sine_table = jnp.sin(angles)
        value_real = weights * cosine_table
        value_imag = -weights * sine_table
        slope_real = -weights * wave_east * sine_table
        slope_imag = -weights * wave_east * cosine_table
        value_table = jnp.stack([value_real, value_imag], axis=1)
        slope_table = jnp.stack([slope_real, slope_imag], axis=1)
        east_table = jnp.stack([value_table, slope_table], axis=3).reshape(
            columns, 2 * local_waves, 2, block_size
        )
        product = jnp.einsum("clyfk,ckab->falyb", stacked, east_table, precision=HIGHEST)
        return lax.dynamic_update_slice_in_dim(result, product, block_index * block_size, 4)

    initial = jnp.zeros((field_count, 2, slot_count, row_count, east_cells), jnp.float32)
    return lax.fori_loop(0, block_count, east_one_block, initial)


def place_levels(grid_all, level_slot):
    slot_count = grid_all.shape[2]
    selector = (level_slot[None, :] == jnp.arange(slot_count, dtype=jnp.int32)[:, None]).astype(
        jnp.float32
    )
    return jnp.einsum("ls,fasyx->falyx", selector, grid_all, precision=HIGHEST)


def plain_on_device(vorticity, divergence, trunc_cut, level_slot):
    columns = lax.axis_size("col")
    row_count = lax.axis_size("row")
    local_waves = vorticity.shape[2]
    north_cells = vorticity.shape[3]
    east_cells = 2 * local_waves * columns
    first_wave = lax.axis_index("col") * local_waves
    spectra = spectral_winds(vorticity, divergence, trunc_cut, first_wave, east_cells)
    slot_count = spectra.shape[0]
    flattened = spectra.reshape(slot_count, 4 * local_waves, north_cells)
    fourier = north_transform(flattened, local_waves)
    outgoing = fourier[None]
    received = lax.all_to_all(outgoing, ("col", "row"), split_axis=2, concat_axis=0, tiled=True)
    shaped = received.reshape(
        columns,
        row_count * received.shape[1],
        received.shape[2],
        received.shape[3],
        received.shape[4],
    )
    grid_all = east_transform(shaped, local_waves, east_cells)
    placed = place_levels(grid_all, level_slot)
    return (placed[0, 0], placed[1, 0], placed[0, 1], placed[1, 1])


def solution(mesh):
    columns = mesh.shape["col"]
    groups = mesh.shape["row"]
    width = 2 if columns % 2 == 0 else 1
    fine = Mesh(mesh.devices.reshape(columns // width, width, groups), ("height", "width", "row"))

    def whole(vorticity, divergence, trunc_cut, level_slot):
        waves = vorticity.shape[2] // columns
        local = jax.ShapeDtypeStruct((2, vorticity.shape[1] // groups, waves, vorticity.shape[3]), F32)
        fast = fast_shapes(fine, local)
        column = ("height", "width") if fast else "col"
        grid = P(None, ("height", "width", "row") if fast else ("col", "row"), None)
        spectral = P(None, "row", column, None)
        return jax.shard_map(
            fast_on_device if fast else plain_on_device,
            mesh=fine if fast else mesh,
            in_specs=(spectral, spectral, P(column), P()),
            out_specs=(grid, grid, grid, grid),
            check_vma=False,
        )(vorticity, divergence, trunc_cut, level_slot)

    return whole
```
